8 devices in a mesh: dp: 1 (over z), cp: 8 (over y, x, core).
Axes of the slice: x: 2, y: 2, z: 1, core: 2. Of those that a mesh axis runs over, the one named last changes fastest.
Arguments:
- x: bfloat16 [2048, 3584], P(('dp', 'cp'))
- seg: int32 [2048], P(('dp', 'cp'))
- wq: bfloat16 [3584, 3584], replicated
- wk: bfloat16 [3584, 512], replicated
- wv: bfloat16 [3584, 512], replicated
- wo: bfloat16 [3584, 3584], replicated
Outputs:
- output: bfloat16 [2048, 3584], P(('dp', 'cp'))
All inputs are finite; a program needn't handle non-finite values.
Results may differ from the reference program's by a relative error of at most 0.00752571.
Values are sent between devices in bfloat16 or wider.
A program may use at most 1 GiB of HBM per device.

```python
import jax
import jax.numpy as jnp
from jax import lax
import numpy as np

CP = 8
L = 256
D = 3584
HQ = 28
HKV = 4
DH = 128

S = CP * L
HALF = L // 2
G = HQ // HKV
QB = min(128, HALF)


def row_positions():
    rows = []
    for d in range(CP):
        rows.append(np.arange(d * HALF, (d + 1) * HALF))
        rows.append(np.arange((2 * CP - 1 - d) * HALF, (2 * CP - d) * HALF))
    return np.concatenate(rows).astype(np.int32)


def setup_inputs(seed: int = 0, part: int = 0) -> dict:
    key = jax.random.key(seed)
    kshared, kpart = jax.random.split(key)
    kp = jax.random.fold_in(kpart, part)
    kx, _, _ = jax.random.split(kp, 3)
    kd = jax.random.fold_in(kp, 7)
    ku, kc, kl = jax.random.split(kd, 3)
    kq, kk, kv, ko = jax.random.split(kshared, 4)
    x = jax.random.normal(kx, (S, D), jnp.float32).astype(jnp.bfloat16)
    token_pos = jnp.arange(S, dtype=jnp.int32)
    long_end = jax.random.randint(kl, (), 3 * S // 10, 7 * S // 10, jnp.int32)
    coin_flip = jax.random.randint(kc, (2 * CP,), 0, 2, jnp.int32)
    break_bar = jnp.repeat(jnp.where(coin_flip == 0, jnp.int32(1 << 22), jnp.int32((1 << 24) // L)), HALF)
    draw_bits = (jax.random.bits(ku, (S,), jnp.uint32) >> 8).astype(jnp.int32)
    breaks = (draw_bits < break_bar) & (token_pos > long_end)
    seg_orig = 7 + jnp.cumsum(breaks.astype(jnp.int32))
    seg = seg_orig[jnp.asarray(row_positions())].astype(jnp.int32)
    wq = (jax.random.normal(kq, (D, HQ * DH), jnp.float32) * (2.0 * D ** -0.5)).astype(jnp.bfloat16)
    wk = (jax.random.normal(kk, (D, HKV * DH), jnp.float32) * D ** -0.5).astype(jnp.bfloat16)
    wv = (jax.random.normal(kv, (D, HKV * DH), jnp.float32) * D ** -0.5).astype(jnp.bfloat16)
    wo = (jax.random.normal(ko, (HQ * DH, D), jnp.float32) * (HQ * DH) ** -0.5).astype(jnp.bfloat16)
    return {"x": x, "seg": seg, "wq": wq, "wk": wk, "wv": wv, "wo": wo}


def reference(x, seg, wq, wk, wv, wo):
    pos = jnp.asarray(row_positions())
    q = jnp.dot(x, wq, preferred_element_type=jnp.float32).astype(jnp.bfloat16)
    k = jnp.dot(x, wk, preferred_element_type=jnp.float32).astype(jnp.bfloat16)
    v = jnp.dot(x, wv, preferred_element_type=jnp.float32).astype(jnp.bfloat16)
    kf = k.astype(jnp.float32).reshape(S, HKV, DH)
    vf = v.astype(jnp.float32).reshape(S, HKV, DH)
    qb = q.reshape(S // QB, QB, HKV, G, DH)
    pb = pos.reshape(S // QB, QB)
    sb = seg.reshape(S // QB, QB)

    def block(args):
        qi, pi, si = args
        s = jnp.einsum("qhgd,khd->hgqk", qi.astype(jnp.float32), kf) * DH ** -0.5
        allowed = (si[:, None] == seg[None, :]) & (pos[None, :] <= pi[:, None])
        s = jnp.where(allowed, s, -jnp.inf)
        p = jax.nn.softmax(s, axis=-1)
        o = jnp.einsum("hgqk,khd->qhgd", p, vf)
        return o.astype(jnp.bfloat16)

    o = lax.map(block, (qb, pb, sb)).reshape(S, HQ * DH)
    return jnp.dot(o, wo, preferred_element_type=jnp.float32).astype(jnp.bfloat16)
```

```python
import functools

import jax
import jax.numpy as jnp
from jax import lax
from jax.experimental import pallas as pl
from jax.experimental.pallas import tpu as pltpu
from jax.sharding import PartitionSpec as P

DH = 128
HALF = 128
KB = 256
NC = 512
MESH = pl.DeviceIdType.MESH
F32 = jnp.float32
BF16 = jnp.bfloat16
LOG2E = 1.4426950408889634


def _kernel(n, g_sz, x_hbm, seg_hbm, wq_hbm, wk_hbm, wv_hbm, wo_hbm, y_hbm,
            x_s, w_s, kv_s, q_s, o_s, s_s, b_s, m_s, l_s, a_s, y_s, yb_s, seg_s, sq_s,
            x_sem, w_sem, o_sem, ss_sem, sr_sem, send_sem, recv_sem, loc_sem):
    me = lax.axis_index("cp")
    c, xx, yy = me % 2, (me // 2) % 2, me // 4

    def dev(dy, dx, dc):
        ny = 1 - yy if dy else yy
        nx = 1 - xx if dx else xx
        nc = 1 - c if dc else c
        return ny * 4 + nx * 2 + nc

    d_model = x_s.shape[1]
    n_q = wq_hbm.shape[1] // NC
    n_kv = wk_hbm.shape[1] // DH
    half_k = d_model // 2
    peers = [dev(k // 4, (k // 2) % 2, k % 2) for k in range(n)]
    sib = peers[1]

    def load(i):
        if i < 2:
            cols = pl.ds(i * 2 * DH, 2 * DH)
            return [
                pltpu.make_async_copy(wk_hbm.at[:, cols], w_s.at[i, :, pl.ds(0, 2 * DH)], w_sem.at[i]),
                pltpu.make_async_copy(wv_hbm.at[:, cols], w_s.at[i, :, pl.ds(2 * DH, 2 * DH)], w_sem.at[n_q * 2 + 2 + i]),
            ]
        if i < 2 + n_q:
            return [pltpu.make_async_copy(wq_hbm.at[:, pl.ds((i - 2) * NC, NC)], w_s.at[i], w_sem.at[i])]
        j = i - 2 - n_q
        return [pltpu.make_async_copy(wo_hbm.at[:, pl.ds(j * NC, NC)], w_s.at[j], w_sem.at[i])]

    def start(i):
        for cp in load(i):
            cp.start()

    def wait(i):
        for cp in load(i):
            cp.wait()

    x_cp = pltpu.make_async_copy(x_hbm, x_s, x_sem)
    seg_cp = pltpu.make_async_copy(seg_hbm, seg_s.at[me], loc_sem)
    x_cp.start()
    seg_cp.start()
    start(0)
    start(1)
    start(2)

    barrier = pltpu.get_barrier_semaphore()
    for k in range(1, n):
        pl.semaphore_signal(barrier, inc=1, device_id={"cp": peers[k]}, device_id_type=MESH)
    pl.semaphore_wait(barrier, n - 1)

    def seg_copy(k):
        return pltpu.make_async_remote_copy(
            src_ref=seg_s.at[me], dst_ref=seg_s.at[me], send_sem=ss_sem.at[k], recv_sem=sr_sem.at[k],
            device_id={"cp": peers[k]}, device_id_type=MESH)

    def seg_recv(k):
        return pltpu.make_async_remote_copy(
            src_ref=seg_s.at[peers[k]], dst_ref=seg_s.at[peers[k]], send_sem=ss_sem.at[k], recv_sem=sr_sem.at[k],
            device_id={"cp": peers[k]}, device_id_type=MESH)

    seg_cp.wait()
    for k in range(1, n):
        seg_copy(k).start()

    own_to = [1, 2, 4, 6]

    def kv_copy(g, role, ab):
        src_dev = me if role < 4 else peers[own_to[role - 3]]
        to = peers[own_to[role]] if role < 4 else sib
        return _chunk(g, role, ab, src_dev, to)

    def kv_recv(g, role, ab):
        src_dev = peers[own_to[role]] if role < 4 else peers[own_to[role - 3] + 1]
        return _chunk(g, role, ab, src_dev, sib)

    def _chunk(g, role, ab, src_dev, to):
        piece = src_dev if ab == 0 else 2 * n - 1 - src_dev
        rows = pl.ds(pl.multiple_of(piece * HALF, HALF), HALF)
        ref = kv_s.at[g, :, rows, :]
        return pltpu.make_async_remote_copy(
            src_ref=ref, dst_ref=ref, send_sem=send_sem.at[g, role, ab], recv_sem=recv_sem.at[g, role, ab],
            device_id={"cp": to}, device_id_type=MESH)

    x_cp.wait()
    for i in range(2):
        wait(i)
        start(3 + i)
        r = jnp.dot(x_s[...], w_s[i], preferred_element_type=F32).astype(BF16)
        for gg in range(2):
            for ab in range(2):
                piece = me if ab == 0 else 2 * n - 1 - me
                rows = pl.ds(pl.multiple_of(piece * HALF, HALF), HALF)
                for t in range(2):
                    lo = t * 2 * DH + gg * DH
                    kv_s[2 * i + gg, t, rows, :] = r[ab * HALF:(ab + 1) * HALF, lo:lo + DH]
        start(2 + n_q + i)
        for gg in range(2):
            for ab in range(2):
                for role in range(4):
                    kv_copy(2 * i + gg, role, ab).start()

    def q_chunk(j):
        r = jnp.dot(x_s[...], w_s[2 + j], preferred_element_type=F32).astype(BF16)
        for hh in range(NC // DH):
            for ab in range(2):
                q_s[ab, j * (NC // DH) + hh] = r[ab * HALF:(ab + 1) * HALF, hh * DH:(hh + 1) * DH]

    for j in range(n_q):
        wait(2 + j)
        if 5 + j < 2 + n_q:
            start(5 + j)
        q_chunk(j)
        if 2 + j < n_q:
            start(4 + n_q + j)

    for k in range(1, n):
        seg_recv(k).wait_recv()
    n_a = me // 2 + 1
    n_t = n + 1
    for ab in range(2):
        row = seg_s[me, pl.ds(ab, 1), :]
        sq_s[ab] = jnp.transpose(jnp.broadcast_to(row, (HALF, HALF)))

    def block_of(t):
        ab = jnp.where(t >= n_a, 1, 0)
        return ab, t - ab * n_a

    def mask_step(t, _):
        ab, kb = block_of(t)
        qp = jnp.where(ab == 1, 2 * n - 1 - me, me)
        pos_q = qp * HALF + lax.broadcasted_iota(jnp.int32, (HALF, HALF), 0)
        for h in range(2):
            p = kb * 2 + h
            hi = jnp.where(p >= n, 1, 0)
            d = jnp.where(p >= n, 2 * n - 1 - p, p)
            sk = seg_s[d, pl.ds(hi, 1), :]
            pos_k = p * HALF + lax.broadcasted_iota(jnp.int32, (HALF, HALF), 1)
            ok = (sq_s[ab] == sk) & (pos_k <= pos_q)
            b_s[t, :, h * HALF:(h + 1) * HALF] = jnp.where(ok, 0.0, -jnp.inf)
        return 0

    lax.fori_loop(0, n_t, mask_step, 0)

    rows_g = g_sz * HALF
    scale = LOG2E * DH ** -0.5

    def attention(g):
        m_s[...] = jnp.full_like(m_s, -jnp.inf)

        def scores(t, _):
            ab, kb = block_of(t)
            q = q_s[ab, pl.ds(g * g_sz, g_sz)].reshape(rows_g, DH)
            k = kv_s[g, 0, pl.ds(pl.multiple_of(kb * KB, KB), KB), :]
            s = lax.dot_general(q, k, (((1,), (1,)), ((), ())), preferred_element_type=F32)
            s = s.reshape(g_sz, HALF, KB)
            for j in range(g_sz):
                sj = s[j] + b_s[t]
                s_s[t, j] = sj
                m_s[ab, j] = jnp.maximum(m_s[ab, j], jnp.maximum(sj[:, :HALF], sj[:, HALF:]))
            return 0

        lax.fori_loop(0, n_t, scores, 0)
        for ab in range(2):
            for j in range(g_sz):
                m_s[ab, j] = jnp.broadcast_to(jnp.max(m_s[ab, j], axis=1, keepdims=True), (HALF, HALF))
        l_s[...] = jnp.zeros_like(l_s)
        a_s[...] = jnp.zeros_like(a_s)

        def values(t, _):
            ab, kb = block_of(t)
            v = kv_s[g, 1, pl.ds(pl.multiple_of(kb * KB, KB), KB), :]
            ps = []
            for j in range(g_sz):
                m = m_s[ab, j]
                p0 = jnp.exp2((s_s[t, j, :, :HALF] - m) * scale)
                p1 = jnp.exp2((s_s[t, j, :, HALF:] - m) * scale)
                l_s[ab, j] += p0 + p1
                ps.append(jnp.concatenate([p0.astype(BF16), p1.astype(BF16)], axis=1))
            p = jnp.concatenate(ps, axis=0)
            a_s[ab] += jnp.dot(p, v, preferred_element_type=F32).reshape(g_sz, HALF, DH)
            return 0

        lax.fori_loop(0, n_t, values, 0)
        for ab in range(2):
            for j in range(g_sz):
                l = jnp.sum(l_s[ab, j], axis=1, keepdims=True)
                o = (a_s[ab, j] / l).astype(BF16)
                cols = pl.ds(pl.multiple_of((g * g_sz + j) * DH, DH), DH)
                o_s[ab * HALF:(ab + 1) * HALF, cols] = o

    def pass_on(g):
        for role in (1, 2, 3):
            for ab in range(2):
                kv_recv(g, role, ab).wait_recv()
                kv_copy(g, role + 3, ab).start()

    def arrived(g):
        for role in (0, 4, 5, 6):
            for ab in range(2):
                kv_recv(g, role, ab).wait_recv()

    pass_on(0)
    for hf in range(2):
        for gg in range(2):
            g = hf * 2 + gg
            if g + 1 < n_kv:
                pass
            arrived(g)
            attention(g)
            if g + 1 < n_kv:
                pass_on(g + 1)

        def out_chunk(j, _):
            o = o_s[:, hf * half_k:(hf + 1) * half_k]
            y = jnp.dot(o, w_s[j, hf * half_k:(hf + 1) * half_k, :], preferred_element_type=F32)
            if hf == 0:
                y_s[j] = y
            else:
                yb_s[j] = (y_s[j] + y).astype(BF16)
            return 0

        for j in range(n_q):
            if hf == 0:
                wait(2 + n_q + j)
            out_chunk(j, 0)
            if hf == 1:
                pltpu.make_async_copy(yb_s.at[j], y_hbm.at[:, pl.ds(j * NC, NC)], o_sem.at[j]).start()

    for j in range(n_q):
        pltpu.make_async_copy(yb_s.at[j], y_hbm.at[:, pl.ds(j * NC, NC)], o_sem.at[j]).wait()
    for k in range(1, n):
        seg_copy(k).wait_send()
    for g in range(n_kv):
        for role in range(7):
            for ab in range(2):
                kv_copy(g, role, ab).wait_send()


def solution(mesh):
    n = mesh.shape["cp"]

    def local(x, seg, wq, wk, wv, wo):
        lq, d = x.shape
        hq = wq.shape[1] // DH
        hkv = wk.shape[1] // DH
        g_sz = hq // hkv
        n_q = wq.shape[1] // NC
        dma = pltpu.SemaphoreType.DMA
        anyspec = pl.BlockSpec(memory_space=pl.ANY)
        return pl.pallas_call(
            functools.partial(_kernel, n, g_sz),
            out_shape=jax.ShapeDtypeStruct((lq, wo.shape[1]), BF16),
            in_specs=[anyspec] * 6,
            out_specs=anyspec,
            scratch_shapes=[
                pltpu.VMEM((lq, d), BF16),
                pltpu.VMEM((n_q + 2, d, NC), BF16),
                pltpu.VMEM((hkv, 2, n * lq, DH), BF16),
                pltpu.VMEM((2, hq, HALF, DH), BF16),
                pltpu.VMEM((lq, hq * DH), BF16),
                pltpu.VMEM((n + 1, g_sz, HALF, KB), F32),
                pltpu.VMEM((n + 1, HALF, KB), F32),
                pltpu.VMEM((2, g_sz, HALF, HALF), F32),
                pltpu.VMEM((2, g_sz, HALF, HALF), F32),
                pltpu.VMEM((2, g_sz, HALF, DH), F32),
                pltpu.VMEM((n_q, lq, NC), F32),
                pltpu.VMEM((n_q, lq, NC), BF16),
                pltpu.VMEM((n, 2, HALF), jnp.int32),
                pltpu.VMEM((2, HALF, HALF), jnp.int32),
                dma, dma((2 * n_q + 4,)), dma((n_q,)), dma((n,)), dma((n,)),
                dma((hkv, 7, 2)), dma((hkv, 7, 2)), dma,
            ],
            compiler_params=pltpu.CompilerParams(
                collective_id=0, has_side_effects=True, vmem_limit_bytes=67043328),
            name="layer",
        )(x, seg.reshape(2, HALF), wq, wk, wv, wo)

    rows = P(("dp", "cp"), None)
    return jax.shard_map(local, mesh=mesh, in_specs=(rows, P(("dp", "cp")), P(), P(), P(), P()), out_specs=rows, check_vma=False)
```

```python
import functools

import jax
import jax.numpy as jnp
from jax import lax
from jax.experimental import pallas as pl
from jax.experimental.pallas import tpu as pltpu
from jax.sharding import PartitionSpec as P

DH = 128
HALF = 128
KB = 256
NC = 512
MESH = pl.DeviceIdType.MESH
F32 = jnp.float32
BF16 = jnp.bfloat16
UNROLL = 3
LOG2E = 1.4426950408889634


def _kernel(n, g_sz, x_hbm, seg_hbm, wq_hbm, wk_hbm, wv_hbm, wo_hbm, y_hbm,
            x_s, w_s, kv_s, q_s, o_s, s_s, b_s, m_s, l_s, a_s, y_s, yb_s, seg_s,
            x_sem, w_sem, o_sem, ss_sem, sr_sem, send_sem, recv_sem, loc_sem):
    me = lax.axis_index("cp")
    c, xx, yy = me % 2, (me // 2) % 2, me // 4

    def dev(dy, dx, dc):
        ny = 1 - yy if dy else yy
        nx = 1 - xx if dx else xx
        nc = 1 - c if dc else c
        return ny * 4 + nx * 2 + nc

    d_model = x_s.shape[1]
    n_q = wq_hbm.shape[1] // NC
    n_kv = wk_hbm.shape[1] // DH
    half_k = d_model // 2
    peers = [dev(k // 4, (k // 2) % 2, k % 2) for k in range(n)]
    sib = peers[1]

    def load(i):
        if i < 2:
            cols = pl.ds(i * 2 * DH, 2 * DH)
            return [
                pltpu.make_async_copy(wk_hbm.at[:, cols], w_s.at[i, :, pl.ds(0, 2 * DH)], w_sem.at[i]),
                pltpu.make_async_copy(wv_hbm.at[:, cols], w_s.at[i, :, pl.ds(2 * DH, 2 * DH)], w_sem.at[n_q * 2 + 2 + i]),
            ]
        if i < 2 + n_q:
            return [pltpu.make_async_copy(wq_hbm.at[:, pl.ds((i - 2) * NC, NC)], w_s.at[i], w_sem.at[i])]
        j = i - 2 - n_q
        return [pltpu.make_async_copy(wo_hbm.at[:, pl.ds(j * NC, NC)], w_s.at[j], w_sem.at[i])]

    def start(i):
        for cp in load(i):
            cp.start()

    def wait(i):
        for cp in load(i):
            cp.wait()

    x_cp = pltpu.make_async_copy(x_hbm, x_s, x_sem)
    seg_cp = pltpu.make_async_copy(seg_hbm, seg_s.at[me], loc_sem)
    x_cp.start()
    seg_cp.start()
    start(0)
    start(1)
    start(2)

    def seg_copy(k):
        return pltpu.make_async_remote_copy(
            src_ref=seg_s.at[me], dst_ref=seg_s.at[me], send_sem=ss_sem.at[k], recv_sem=sr_sem.at[k],
            device_id={"cp": peers[k]}, device_id_type=MESH)

    def seg_recv(k):
        return pltpu.make_async_remote_copy(
            src_ref=seg_s.at[peers[k]], dst_ref=seg_s.at[peers[k]], send_sem=ss_sem.at[k], recv_sem=sr_sem.at[k],
            device_id={"cp": peers[k]}, device_id_type=MESH)

    barrier = pltpu.get_barrier_semaphore()
    for k in range(1, n):
        pl.semaphore_signal(barrier, inc=1, device_id={"cp": peers[k]}, device_id_type=MESH)

    own_to = [1, 2, 4, 6]

    def kv_copy(g, role, ab):
        if role < 3:
            src_dev, to = me, peers[own_to[role]]
        elif role == 3:
            src_dev, to = (peers[2], peers[4]) if ab == 0 else (peers[4], peers[2])
        else:
            src_dev, to = peers[own_to[role - 3]], sib
        return _chunk(g, role, ab, src_dev, to)

    def kv_recv(g, role, ab):
        src_dev = peers[own_to[role]] if role < 4 else peers[own_to[role - 3] + 1]
        return _chunk(g, role, ab, src_dev, sib)

    def _chunk(g, role, ab, src_dev, to):
        ref = kv_s.at[g, src_dev if ab == 0 else 2 * n - 1 - src_dev]
        return pltpu.make_async_remote_copy(
            src_ref=ref, dst_ref=ref, send_sem=send_sem.at[g, role, ab], recv_sem=recv_sem.at[g, role, ab],
            device_id={"cp": to}, device_id_type=MESH)

    def send_own(g):
        for role in (1, 2, 0):
            for ab in range(2):
                kv_copy(g, role, ab).start()

    def forward(g):
        for ab in range(2):
            for role in (1, 2):
                kv_recv(g, role, ab).wait_recv()
        for ab in range(2):
            kv_copy(g, 3, ab).start()
        for ab in range(2):
            for role in (4, 5):
                kv_copy(g, role, ab).start()

    def forward_diag(g):
        for ab in range(2):
            kv_recv(g, 3, ab).wait_recv()
        for ab in range(2):
            kv_copy(g, 6, ab).start()

    def arrived(g):
        for role in (0, 4, 5, 6):
            for ab in range(2):
                kv_recv(g, role, ab).wait_recv()

    x_cp.wait()
    for i in range(2):
        wait(i)
        start(3 + i)
        r = jnp.dot(x_s[...], w_s[i], preferred_element_type=F32)
        for gg in range(2):
            for ab in range(2):
                piece = me if ab == 0 else 2 * n - 1 - me
                part = r[ab * HALF:(ab + 1) * HALF]
                kv_s[2 * i + gg, piece, 0] = part[:, gg * DH:(gg + 1) * DH].astype(BF16)
                v = part[:, (2 + gg) * DH:(3 + gg) * DH]
                kv_s[2 * i + gg, piece, 1] = jnp.transpose(v).astype(BF16)
        if i == 0:
            pl.semaphore_wait(barrier, n - 1)
            send_own(0)
            send_own(1)
            seg_cp.wait()
            for k in range(1, n):
                seg_copy(k).start()

    def q_chunk(j):
        r = jnp.dot(x_s[...], w_s[2 + j], preferred_element_type=F32).astype(BF16)
        for hh in range(NC // DH):
            for ab in range(2):
                q_s[ab, j * (NC // DH) + hh] = r[ab * HALF:(ab + 1) * HALF, hh * DH:(hh + 1) * DH]

    for j in range(n_q):
        wait(2 + j)
        start(5 + j)
        q_chunk(j)
        if j == 2:
            forward(0)
            send_own(2)
        if j == 5:
            forward(1)
            send_own(3)
        if j == 6:
            forward_diag(0)
    for j in range(5 + n_q, 2 + 2 * n_q):
        start(j)

    for k in range(1, n):
        seg_recv(k).wait_recv()
    n_a = me // 2 + 1
    n_t = n + 1
    def block_of(t):
        ab = jnp.where(t >= n_a, 1, 0)
        return ab, t - ab * n_a

    def mask_step(t, _):
        ab, kb = block_of(t)
        qp = jnp.where(ab == 1, 2 * n - 1 - me, me)
        sq = seg_s[me, pl.ds(ab, 1), :]
        pos_q = qp * HALF + lax.broadcasted_iota(jnp.int32, (HALF, HALF), 1)
        for h in range(2):
            p = kb * 2 + h
            hi = jnp.where(p >= n, 1, 0)
            d = jnp.where(p >= n, 2 * n - 1 - p, p)
            sk = jnp.transpose(jnp.broadcast_to(seg_s[d, pl.ds(hi, 1), :], (HALF, HALF)))
            pos_k = p * HALF + lax.broadcasted_iota(jnp.int32, (HALF, HALF), 0)
            ok = (sk == sq) & (pos_k <= pos_q)
            b_s[t, h * HALF:(h + 1) * HALF, :] = jnp.where(ok, 0.0, -jnp.inf)
        return 0

    lax.fori_loop(0, n_t, mask_step, 0)

    rows_g = g_sz * HALF
    scale = LOG2E * DH ** -0.5
    sub = KB // 8

    def fold(op, a):
        return op(a.reshape(sub, 8, HALF), axis=0)

    def attention(g):
        m_s[...] = jnp.full_like(m_s, -jnp.inf)
        l_s[...] = jnp.zeros_like(l_s)
        a_s[...] = jnp.zeros_like(a_s)

        def scores(t):
            ab, kb = block_of(t)
            q = q_s[ab, pl.ds(g * g_sz, g_sz)].reshape(rows_g, DH)
            k = kv_s[g, pl.ds(kb * 2, 2), 0].reshape(KB, DH)
            s = lax.dot_general(k, q, (((1,), (1,)), ((), ())), preferred_element_type=F32)
            for j in range(g_sz):
                sj = s[:, j * HALF:(j + 1) * HALF] + b_s[t]
                s_s[t, j] = sj
                m_s[ab, j] = jnp.maximum(m_s[ab, j], fold(jnp.max, sj))

        def values(t):
            ab, kb = block_of(t)
            v = jnp.concatenate([kv_s[g, kb * 2, 1], kv_s[g, kb * 2 + 1, 1]], axis=1)
            ps = []
            for j in range(g_sz):
                p = jnp.exp2((s_s[t, j].reshape(sub, 8, HALF) - m_s[ab, j][None]) * scale)
                l_s[ab, j] += jnp.sum(p, axis=0)
                ps.append(p.reshape(KB, HALF).astype(BF16))
            p = jnp.concatenate(ps, axis=1)
            a_s[ab] += jnp.dot(v, p, preferred_element_type=F32)

        def loop(f):
            def body(i, _):
                for u in range(UNROLL):
                    f(i * UNROLL + u)
                return 0
            lax.fori_loop(0, n_t // UNROLL, body, 0)

        loop(scores)
        m_s[...] = jnp.broadcast_to(jnp.max(m_s[...], axis=2, keepdims=True), m_s.shape)
        loop(values)
        for ab in range(2):
            for j in range(g_sz):
                l = jnp.sum(l_s[ab, j], axis=0, keepdims=True)
                o = jnp.transpose(a_s[ab, :, j * HALF:(j + 1) * HALF] / l).astype(BF16)
                o_s[ab * HALF:(ab + 1) * HALF, (g * g_sz + j) * DH:(g * g_sz + j + 1) * DH] = o

    for hf in range(2):
        for gg in range(2):
            g = hf * 2 + gg
            arrived(g)
            attention(g)
            if g == 0:
                forward(2)
                forward_diag(1)
            if g == 1:
                forward(3)

        for j in range(n_q):
            if hf == 0:
                wait(2 + n_q + j)
            o = o_s[:, hf * half_k:(hf + 1) * half_k]
            y = jnp.dot(o, w_s[j, hf * half_k:(hf + 1) * half_k, :], preferred_element_type=F32)
            if hf == 0:
                y_s[j] = y
                if j == 1:
                    forward_diag(2)
                if j == 4:
                    forward_diag(3)
            else:
                yb_s[j] = (y_s[j] + y).astype(BF16)
                pltpu.make_async_copy(yb_s.at[j], y_hbm.at[:, pl.ds(j * NC, NC)], o_sem.at[j]).start()

    for j in range(n_q):
        pltpu.make_async_copy(yb_s.at[j], y_hbm.at[:, pl.ds(j * NC, NC)], o_sem.at[j]).wait()
    for k in range(1, n):
        seg_copy(k).wait_send()
    for g in range(n_kv):
        for role in range(7):
            for ab in range(2):
                kv_copy(g, role, ab).wait_send()


def solution(mesh):
    n = mesh.shape["cp"]

    def local(x, seg, wq, wk, wv, wo):
        lq, d = x.shape
        hq = wq.shape[1] // DH
        hkv = wk.shape[1] // DH
        g_sz = hq // hkv
        n_q = wq.shape[1] // NC
        dma = pltpu.SemaphoreType.DMA
        anyspec = pl.BlockSpec(memory_space=pl.ANY)
        return pl.pallas_call(
            functools.partial(_kernel, n, g_sz),
            out_shape=jax.ShapeDtypeStruct((lq, wo.shape[1]), BF16),
            in_specs=[anyspec] * 6,
            out_specs=anyspec,
            scratch_shapes=[
                pltpu.VMEM((lq, d), BF16),
                pltpu.VMEM((n_q + 2, d, NC), BF16),
                pltpu.VMEM((hkv, 2 * n, 2, HALF, DH), BF16),
                pltpu.VMEM((2, hq, HALF, DH), BF16),
                pltpu.VMEM((lq, hq * DH), BF16),
                pltpu.VMEM((n + 1, g_sz, KB, HALF), F32),
                pltpu.VMEM((n + 1, KB, HALF), F32),
                pltpu.VMEM((2, g_sz, 8, HALF), F32),
                pltpu.VMEM((2, g_sz, 8, HALF), F32),
                pltpu.VMEM((2, DH, g_sz * HALF), F32),
                pltpu.VMEM((n_q, lq, NC), F32),
                pltpu.VMEM((n_q, lq, NC), BF16),
                pltpu.VMEM((n, 2, HALF), jnp.int32),
                dma, dma((2 * n_q + 4,)), dma((n_q,)), dma((n,)), dma((n,)),
                dma((hkv, 7, 2)), dma((hkv, 7, 2)), dma,
            ],
            compiler_params=pltpu.CompilerParams(
                collective_id=0, has_side_effects=True, vmem_limit_bytes=67043328),
            name="layer",
        )(x, seg.reshape(2, HALF), wq, wk, wv, wo)

    rows = P(("dp", "cp"), None)
    return jax.shard_map(local, mesh=mesh, in_specs=(rows, P(("dp", "cp")), P(), P(), P(), P()), out_specs=rows, check_vma=False)
```

```python
import functools

import jax
import jax.numpy as jnp
from jax import lax
from jax.experimental import pallas as pl
from jax.experimental.pallas import tpu as pltpu
from jax.sharding import PartitionSpec as P

DH = 128
HALF = 128
KB = 256
NC = 512
MESH = pl.DeviceIdType.MESH
F32 = jnp.float32
BF16 = jnp.bfloat16
LOG2E = 1.4426950408889634


def _kernel(n, g_sz, x_hbm, seg_hbm, wq_hbm, wk_hbm, wv_hbm, wo_hbm, y_ref,
            x_s, w_s, kv_s, q_s, o_s, s_s, b_s, m_s, l_s, a_s, ml_s, ll_s, al_s, y_s, seg_s,
            x_sem, w_sem, ss_sem, sr_sem, send_sem, rn_sem, rd_sem, rs_sem, loc_sem):
    me = lax.axis_index("cp")
    c, xx, yy = me % 2, (me // 2) % 2, me // 4

    def dev(dy, dx, dc):
        ny = 1 - yy if dy else yy
        nx = 1 - xx if dx else xx
        nc = 1 - c if dc else c
        return ny * 4 + nx * 2 + nc

    d_model = x_s.shape[1]
    n_q = wq_hbm.shape[1] // NC
    n_kv = wk_hbm.shape[1] // DH
    half_k = d_model // 2
    peers = [dev(k // 4, (k // 2) % 2, k % 2) for k in range(n)]
    sib = peers[1]

    def load(i):
        if i < 2:
            cols = pl.ds(i * 2 * DH, 2 * DH)
            return [
                pltpu.make_async_copy(wk_hbm.at[:, cols], w_s.at[i, :, pl.ds(0, 2 * DH)], w_sem.at[i]),
                pltpu.make_async_copy(wv_hbm.at[:, cols], w_s.at[i, :, pl.ds(2 * DH, 2 * DH)], w_sem.at[n_q * 2 + 2 + i]),
            ]
        if i < 2 + n_q:
            return [pltpu.make_async_copy(wq_hbm.at[:, pl.ds((i - 2) * NC, NC)], w_s.at[i], w_sem.at[i])]
        j = i - 2 - n_q
        return [pltpu.make_async_copy(wo_hbm.at[:, pl.ds(j * NC, NC)], w_s.at[j], w_sem.at[i])]

    def start(i):
        for cp in load(i):
            cp.start()

    def wait(i):
        for cp in load(i):
            cp.wait()

    x_cp = pltpu.make_async_copy(x_hbm, x_s, x_sem)
    seg_cp = pltpu.make_async_copy(seg_hbm, seg_s.at[me], loc_sem)
    x_cp.start()
    start(0)
    seg_cp.start()

    def seg_copy(k):
        return pltpu.make_async_remote_copy(
            src_ref=seg_s.at[me], dst_ref=seg_s.at[me], send_sem=ss_sem, recv_sem=sr_sem,
            device_id={"cp": peers[k]}, device_id_type=MESH)

    def seg_all():
        ref = seg_s.at[pl.ds(0, n - 1)]
        return pltpu.make_async_remote_copy(
            src_ref=ref, dst_ref=ref, send_sem=ss_sem, recv_sem=sr_sem,
            device_id={"cp": sib}, device_id_type=MESH)

    barrier = pltpu.get_barrier_semaphore()
    for k in range(1, n):
        pl.semaphore_signal(barrier, inc=1, device_id={"cp": peers[k]}, device_id_type=MESH)

    xn, yn, dg = peers[2], peers[4], peers[6]
    first, second = xn * (1 - c) + yn * c, yn * (1 - c) + xn * c

    def chunk(u, src_dev, to, recv):
        ab, g = u // n_kv, u % n_kv
        ref = kv_s.at[g, src_dev if ab == 0 else 2 * n - 1 - src_dev]
        return pltpu.make_async_remote_copy(
            src_ref=ref, dst_ref=ref, send_sem=send_sem, recv_sem=recv.at[u],
            device_id={"cp": to}, device_id_type=MESH)

    def wait_chunks(u, count, recv):
        ref = kv_s.at[u % n_kv, pl.ds(0, count)]
        pltpu.make_async_remote_copy(
            src_ref=ref, dst_ref=ref, send_sem=send_sem, recv_sem=recv.at[u],
            device_id={"cp": sib}, device_id_type=MESH).wait_recv()

    def own(u):
        chunk(u, me, xn, rn_sem).start()
        chunk(u, me, yn, rn_sem).start()
        chunk(u, me, sib, rs_sem).start()

    def forward(u):
        wait_chunks(u, 2, rn_sem)
        chunk(u, first, second, rd_sem).start()
        chunk(u, xn, sib, rs_sem).start()
        chunk(u, yn, sib, rs_sem).start()

    def diag(u):
        wait_chunks(u, 1, rd_sem)
        chunk(u, dg, sib, rs_sem).start()

    def arrived(u):
        wait_chunks(u, 4, rs_sem)

    def hook(name, *acts):
        with jax.named_scope(name):
            for act, u in acts:
                act(u)

    with jax.named_scope("wait_x"):
        x_cp.wait()
        start(1)
    for i in range(2):
        with jax.named_scope(f"wait_kv#i={i}"):
            wait(i)
            if i == 0:
                start(2)
            start(3 + i)
        with jax.named_scope(f"kv#i={i}"):
            r = jnp.dot(x_s[...], w_s[i], preferred_element_type=F32)
            for gg in range(2):
                for ab in range(2):
                    piece = me if ab == 0 else 2 * n - 1 - me
                    part = r[ab * HALF:(ab + 1) * HALF]
                    kv_s[2 * i + gg, piece, 0] = part[:, gg * DH:(gg + 1) * DH].astype(BF16)
                    v = part[:, (2 + gg) * DH:(3 + gg) * DH]
                    kv_s[2 * i + gg, piece, 1] = jnp.transpose(v).astype(BF16)
        if i == 0:
            with jax.named_scope("barrier"):
                pl.semaphore_wait(barrier, n - 1)
                own(0)
                own(1)
                seg_cp.wait()
                for k in range(1, n):
                    seg_copy(k).start()
        else:
            own(2)

    def q_chunk(j):
        r = jnp.dot(x_s[...], w_s[2 + j], preferred_element_type=F32).astype(BF16)
        for hh in range(NC // DH):
            for ab in range(2):
                q_s[ab, j * (NC // DH) + hh] = r[ab * HALF:(ab + 1) * HALF, hh * DH:(hh + 1) * DH]

    for j in range(n_q):
        with jax.named_scope(f"wait_q#j={j}"):
            wait(2 + j)
            start(5 + j)
        with jax.named_scope(f"q#j={j}"):
            q_chunk(j)
        if j == 2:
            hook("hookA", (forward, 0), (own, 3))
        if j == 4:
            hook("hookB", (forward, 1), (own, 4))
        if j == 5:
            hook("hookC", (diag, 0))
        if j == 6:
            hook("hookD", (forward, 2), (own, 5))
    for j in range(5 + n_q, 2 + 2 * n_q):
        start(j)

    n_l = n // 2
    n_h = n_l + 1
    n_a = me // 2 + 1

    def mixed(t):
        ab = jnp.where(t >= n_a, 1, 0)
        return ab, t + ab * (n_l - n_a)

    def mask_step(t, _):
        ab, kb = mixed(t - n_l)
        ab = jnp.where(t < n_l, 1, ab)
        kb = jnp.where(t < n_l, t, kb)
        qp = jnp.where(ab == 1, 2 * n - 1 - me, me)
        sq = seg_s[me, pl.ds(ab, 1), :]
        pos_q = qp * HALF + lax.broadcasted_iota(jnp.int32, (HALF, HALF), 1)
        for h in range(2):
            p = kb * 2 + h
            hi = jnp.where(p >= n, 1, 0)
            d = jnp.where(p >= n, 2 * n - 1 - p, p)
            sk = jnp.transpose(jnp.broadcast_to(seg_s[d, pl.ds(hi, 1), :], (HALF, HALF)))
            pos_k = p * HALF + lax.broadcasted_iota(jnp.int32, (HALF, HALF), 0)
            ok = (sk == sq) & (pos_k <= pos_q)
            b_s[t, h * HALF:(h + 1) * HALF, :] = jnp.where(ok, 0.0, -jnp.inf)
        return 0

    with jax.named_scope("mask"):
        seg_all().wait_recv()
        lax.fori_loop(0, n_l + n_h, mask_step, 0)
        diag(1)

    rows_g = g_sz * HALF
    scale = LOG2E * DH ** -0.5
    neg = -jnp.inf

    def fold(op, a):
        return op(a.reshape(a.shape[0] // 8, 8, HALF), axis=0)

    def across(op, a):
        return jnp.broadcast_to(op(a, axis=0, keepdims=True), a.shape)

    def heads(s, j):
        return s[:, j * HALF:(j + 1) * HALF]

    def probs(s, m):
        return jnp.exp2((s.reshape(s.shape[0] // 8, 8, HALF) - m[None]) * scale).reshape(s.shape)

    def low(g):
        q = q_s[1, g * g_sz:(g + 1) * g_sz].reshape(rows_g, DH)
        k = kv_s[g, 0:n, 0].reshape(n_l * KB, DH)
        s = lax.dot_general(k, q, (((1,), (1,)), ((), ())), preferred_element_type=F32)
        for j in range(g_sz):
            mx = None
            for t in range(n_l):
                sj = heads(s[t * KB:(t + 1) * KB], j) + b_s[t]
                s_s[t, j] = sj
                f = fold(jnp.max, sj)
                mx = f if mx is None else jnp.maximum(mx, f)
            ml_s[g, j] = across(jnp.max, mx)
        v = jnp.concatenate([kv_s[g, p, 1] for p in range(n)], axis=1)
        ps = []
        for j in range(g_sz):
            m = ml_s[g, j]
            m = jnp.where(m == neg, 0.0, m)
            cols, tot = [], None
            for t in range(n_l):
                p = probs(s_s[t, j], m)
                f = fold(jnp.sum, p)
                tot = f if tot is None else tot + f
                cols.append(p.astype(BF16))
            ll_s[g, j] = tot
            ps.append(jnp.concatenate(cols, axis=0))
        al_s[g] = jnp.dot(v, jnp.concatenate(ps, axis=1), preferred_element_type=F32)

    def rest(g):
        for j in range(g_sz):
            m_s[0, j] = jnp.full((8, HALF), neg, F32)
            m_s[1, j] = ml_s[g, j]
        with jax.named_scope(f"hscores#g={g}"):
            for t in range(n_h):
                ab, kb = mixed(t)
                q = q_s[ab, g * g_sz:(g + 1) * g_sz].reshape(rows_g, DH)
                k = kv_s[g, pl.ds(kb * 2, 2), 0].reshape(KB, DH)
                s = lax.dot_general(k, q, (((1,), (1,)), ((), ())), preferred_element_type=F32)
                for j in range(g_sz):
                    sj = heads(s, j) + b_s[n_l + t]
                    s_s[t, j] = sj
                    m_s[ab, j] = jnp.maximum(m_s[ab, j], fold(jnp.max, sj))
        for ab in range(2):
            for j in range(g_sz):
                m_s[ab, j] = across(jnp.max, m_s[ab, j])
        for j in range(g_sz):
            corr = jnp.exp2((ml_s[g, j] - m_s[1, j]) * scale)
            l_s[0, j] = jnp.zeros((8, HALF), F32)
            l_s[1, j] = ll_s[g, j] * corr
            a = heads(al_s[g], j)
            a_s[1, :, j * HALF:(j + 1) * HALF] = (a.reshape(DH // 8, 8, HALF) * corr[None]).reshape(DH, HALF)
        a_s[0] = jnp.zeros((DH, rows_g), F32)
        with jax.named_scope(f"hvalues#g={g}"):
            for t in range(n_h):
                ab, kb = mixed(t)
                v = jnp.concatenate([kv_s[g, kb * 2, 1], kv_s[g, kb * 2 + 1, 1]], axis=1)
                ps = []
                for j in range(g_sz):
                    p = probs(s_s[t, j], m_s[ab, j])
                    l_s[ab, j] += fold(jnp.sum, p)
                    ps.append(p.astype(BF16))
                a_s[ab] += jnp.dot(v, jnp.concatenate(ps, axis=1), preferred_element_type=F32)
        for ab in range(2):
            for j in range(g_sz):
                l = jnp.sum(l_s[ab, j], axis=0, keepdims=True)
                o = jnp.transpose(heads(a_s[ab], j) / l).astype(BF16)
                o_s[ab * HALF:(ab + 1) * HALF, (g * g_sz + j) * DH:(g * g_sz + j + 1) * DH] = o

    after_low = [
        [(forward, 3), (own, 6), (diag, 2)],
        [(forward, 4), (own, 7), (diag, 3)],
        [(forward, 5), (diag, 4)],
        [(forward, 6), (diag, 5)],
    ]
    after_rest = [[(forward, 7)], [(diag, 6)], [], []]
    for g in range(n_kv):
        hook(f"arrived_low#g={g}", (arrived, g))
        with jax.named_scope(f"low#g={g}"):
            low(g)
        hook(f"hook_low#g={g}", *after_low[g])

    for hf in range(2):
        for gg in range(2):
            g = hf * 2 + gg
            hook(f"arrived_high#g={g}", (arrived, n_kv + g))
            with jax.named_scope(f"rest#g={g}"):
                rest(g)
            hook(f"hook_rest#g={g}", *after_rest[g])
        if hf == 0:
            with jax.named_scope("wait_wo"):
                for j in range(n_q):
                    wait(2 + n_q + j)
        with jax.named_scope(f"wo#h={hf}"):
            for j in range(n_q):
                o = o_s[:, hf * half_k:(hf + 1) * half_k]
                y = jnp.dot(o, w_s[j, hf * half_k:(hf + 1) * half_k, :], preferred_element_type=F32)
                if hf == 0:
                    y_s[j] = y
                else:
                    y_ref[:, j * NC:(j + 1) * NC] = (y_s[j] + y).astype(BF16)
        if hf == 0:
            hook("hook_wo", (diag, 7))

    with jax.named_scope("tail"):
        seg_all().wait_send()
        ref = kv_s.at[:, pl.ds(0, 2 * (n - 1))]
        pltpu.make_async_remote_copy(
            src_ref=ref, dst_ref=ref, send_sem=send_sem, recv_sem=rs_sem.at[0],
            device_id={"cp": sib}, device_id_type=MESH).wait_send()


def solution(mesh):
    n = mesh.shape["cp"]

    def local(x, seg, wq, wk, wv, wo):
        lq, d = x.shape
        hq = wq.shape[1] // DH
        hkv = wk.shape[1] // DH
        g_sz = hq // hkv
        n_q = wq.shape[1] // NC
        dma = pltpu.SemaphoreType.DMA
        anyspec = pl.BlockSpec(memory_space=pl.ANY)
        return pl.pallas_call(
            functools.partial(_kernel, n, g_sz),
            out_shape=pltpu.VMEM((lq, wo.shape[1]), BF16),
            in_specs=[anyspec] * 6,
            out_specs=pl.BlockSpec(memory_space=pltpu.VMEM),
            scratch_shapes=[
                pltpu.VMEM((lq, d), BF16),
                pltpu.VMEM((n_q + 2, d, NC), BF16),
                pltpu.VMEM((hkv, 2 * n, 2, HALF, DH), BF16),
                pltpu.VMEM((2, hq, HALF, DH), BF16),
                pltpu.VMEM((lq, hq * DH), BF16),
                pltpu.VMEM((n // 2 + 1, g_sz, KB, HALF), F32),
                pltpu.VMEM((n + 1, KB, HALF), F32),
                pltpu.VMEM((2, g_sz, 8, HALF), F32),
                pltpu.VMEM((2, g_sz, 8, HALF), F32),
                pltpu.VMEM((2, DH, g_sz * HALF), F32),
                pltpu.VMEM((hkv, g_sz, 8, HALF), F32),
                pltpu.VMEM((hkv, g_sz, 8, HALF), F32),
                pltpu.VMEM((hkv, DH, g_sz * HALF), F32),
                pltpu.VMEM((n_q, lq, NC), F32),
                pltpu.VMEM((n, 2, HALF), jnp.int32),
                dma, dma((2 * n_q + 4,)), dma, dma,
                dma, dma((2 * hkv,)), dma((2 * hkv,)), dma((2 * hkv,)), dma,
            ],
            compiler_params=pltpu.CompilerParams(
                collective_id=0, has_side_effects=True, vmem_limit_bytes=60 * 2 ** 20),
            name="layer",
        )(x, seg.reshape(2, HALF), wq, wk, wv, wo)

    rows = P(("dp", "cp"), None)
    return jax.shard_map(local, mesh=mesh, in_specs=(rows, P(("dp", "cp")), P(), P(), P(), P()), out_specs=rows, check_vma=False)
```

```python
import functools

import jax
import jax.numpy as jnp
from jax import lax
from jax.experimental import pallas as pl
from jax.experimental.pallas import tpu as pltpu
from jax.sharding import PartitionSpec as P

DH = 128
HALF = 128
KB = 256
NC = 512
MESH = pl.DeviceIdType.MESH
F32 = jnp.float32
BF16 = jnp.bfloat16
LOG2E = 1.4426950408889634


def _kernel(n, g_sz, x_hbm, seg_hbm, wq_hbm, wk_hbm, wv_hbm, wo_hbm, y_ref,
            x_s, w_s, kv_s, q_s, o_s, s_s, b_s, m_s, l_s, a_s, ml_s, ll_s, al_s, y_s, seg_s,
            x_sem, w_sem, ss_sem, sr_sem, send_sem, rn_sem, rd_sem, rs_sem, loc_sem):
    me = lax.axis_index("cp")
    c, xx, yy = me % 2, (me // 2) % 2, me // 4

    def dev(dy, dx, dc):
        ny = 1 - yy if dy else yy
        nx = 1 - xx if dx else xx
        nc = 1 - c if dc else c
        return ny * 4 + nx * 2 + nc

    d_model = x_s.shape[1]
    n_q = wq_hbm.shape[1] // NC
    n_kv = wk_hbm.shape[1] // DH
    half_k = d_model // 2
    peers = [dev(k // 4, (k // 2) % 2, k % 2) for k in range(n)]
    sib = peers[1]

    def load(i):
        if i < n_kv:
            cols = pl.ds(i * DH, DH)
            slot, lo = i // 2, (i % 2) * 2 * DH
            return [
                pltpu.make_async_copy(wk_hbm.at[:, cols], w_s.at[slot, :, pl.ds(lo, DH)], w_sem.at[i]),
                pltpu.make_async_copy(wv_hbm.at[:, cols], w_s.at[slot, :, pl.ds(lo + DH, DH)], w_sem.at[n_kv + 2 * n_q + i]),
            ]
        j = i - n_kv
        if j < n_q:
            return [pltpu.make_async_copy(wq_hbm.at[:, pl.ds(j * NC, NC)], w_s.at[2 + j], w_sem.at[i])]
        j = j - n_q
        return [pltpu.make_async_copy(wo_hbm.at[:, pl.ds(j * NC, NC)], w_s.at[j], w_sem.at[i])]

    def start(i):
        for cp in load(i):
            cp.start()

    def wait(i):
        for cp in load(i):
            cp.wait()

    x_cp = pltpu.make_async_copy(x_hbm, x_s, x_sem)
    seg_cp = pltpu.make_async_copy(seg_hbm, seg_s.at[me], loc_sem)
    x_cp.start()
    start(0)
    seg_cp.start()

    def seg_copy(k):
        return pltpu.make_async_remote_copy(
            src_ref=seg_s.at[me], dst_ref=seg_s.at[me], send_sem=ss_sem, recv_sem=sr_sem,
            device_id={"cp": peers[k]}, device_id_type=MESH)

    def seg_all():
        ref = seg_s.at[pl.ds(0, n - 1)]
        return pltpu.make_async_remote_copy(
            src_ref=ref, dst_ref=ref, send_sem=ss_sem, recv_sem=sr_sem,
            device_id={"cp": sib}, device_id_type=MESH)

    barrier = pltpu.get_barrier_semaphore()
    for k in range(1, n):
        pl.semaphore_signal(barrier, inc=1, device_id={"cp": peers[k]}, device_id_type=MESH)

    xn, yn, dg = peers[2], peers[4], peers[6]
    first, second = xn * (1 - c) + yn * c, yn * (1 - c) + xn * c

    units = [(ab, 2 * hf + gg) for hf in range(n_kv // 2) for ab in range(2) for gg in range(2)]

    def chunk(u, src_dev, to, recv):
        ab, g = units[u]
        ref = kv_s.at[g, src_dev if ab == 0 else 2 * n - 1 - src_dev]
        return pltpu.make_async_remote_copy(
            src_ref=ref, dst_ref=ref, send_sem=send_sem, recv_sem=recv.at[u],
            device_id={"cp": to}, device_id_type=MESH)

    def wait_chunks(u, count, recv):
        ref = kv_s.at[u % n_kv, pl.ds(0, count)]
        pltpu.make_async_remote_copy(
            src_ref=ref, dst_ref=ref, send_sem=send_sem, recv_sem=recv.at[u],
            device_id={"cp": sib}, device_id_type=MESH).wait_recv()

    def own(u):
        chunk(u, me, xn, rn_sem).start()
        chunk(u, me, yn, rn_sem).start()
        chunk(u, me, sib, rs_sem).start()

    def forward(u):
        wait_chunks(u, 2, rn_sem)
        chunk(u, first, second, rd_sem).start()
        chunk(u, xn, sib, rs_sem).start()
        chunk(u, yn, sib, rs_sem).start()

    def diag(u):
        wait_chunks(u, 1, rd_sem)
        chunk(u, dg, sib, rs_sem).start()

    def arrived(u):
        wait_chunks(u, 4, rs_sem)

    f, d, o = forward, diag, own
    table = {
        "q0": ([], [(f, 0), (o, 3)]),
        "q2": ([], [(f, 1)]),
        "q3": ([(f, 0), (o, 3)], [(f, 2), (o, 4), (d, 0)]),
        "q4": ([(f, 1)], [(f, 3), (o, 5)]),
        "q5": ([(f, 2), (o, 4)], [(d, 1)]),
        "q6": ([(d, 0)], [(d, 2)]),
        "mask": ([(f, 3), (o, 5), (d, 1)], [(f, 4), (o, 6)]),
        "s0": ([(d, 2)], [(d, 3)]),
        "s1": ([(f, 4), (o, 6), (d, 3)], [(f, 5), (o, 7)]),
        "s2": ([], [(d, 4)]),
        "s3": ([(f, 5), (o, 7), (d, 4)], [(f, 6), (d, 5)]),
        "s4": ([(f, 6), (d, 5)], [(f, 7)]),
        "wo0": ([(f, 7), (d, 6)], [(d, 6), (d, 7)]),
        "s5": ([(d, 7)], []),
    }

    def slot(name):
        early, late = table.get(name, ([], []))
        for cond, acts in ((me < 2, early), (me >= 2, late)):
            if acts:
                @pl.when(cond)
                def _():
                    with jax.named_scope(f"slot_{name}"):
                        for act, u in acts:
                            act(u)

    with jax.named_scope("wait_x"):
        x_cp.wait()
        start(1)
    for g in range(n_kv):
        with jax.named_scope(f"wait_kv#g={g}"):
            wait(g)
            if g == 0:
                start(2)
                start(3)
            else:
                start(n_kv + g - 1)
        with jax.named_scope(f"kv#g={g}"):
            lo = (g % 2) * 2 * DH
            r = sum(jnp.dot(x_s[:, h * half_k:(h + 1) * half_k], w_s[g // 2, h * half_k:(h + 1) * half_k, lo:lo + 2 * DH],
                            preferred_element_type=F32) for h in range(2))
            for ab in range(2):
                piece = me if ab == 0 else 2 * n - 1 - me
                part = r[ab * HALF:(ab + 1) * HALF]
                kv_s[g, piece, 0] = part[:, :DH].astype(BF16)
                kv_s[g, piece, 1] = jnp.transpose(part[:, DH:]).astype(BF16)
        for cond, acts in ((me >= 2, {0: [0], 1: [1, 2]}), (me < 2, {2: [0, 1, 2]})):
            if g in acts:
                @pl.when(cond)
                def _():
                    if acts[g][0] == 0:
                        with jax.named_scope("barrier"):
                            pl.semaphore_wait(barrier, n - 1)
                    for u in acts[g]:
                        own(u)
                    if acts[g][0] == 0:
                        seg_cp.wait()
                        for k in range(1, n):
                            seg_copy(k).start()

    def q_chunk(j):
        r = jnp.dot(x_s[...], w_s[2 + j], preferred_element_type=F32).astype(BF16)
        for hh in range(NC // DH):
            for ab in range(2):
                q_s[ab, j * (NC // DH) + hh] = r[ab * HALF:(ab + 1) * HALF, hh * DH:(hh + 1) * DH]

    for j in range(n_q):
        with jax.named_scope(f"wait_q#j={j}"):
            wait(n_kv + j)
            start(n_kv + j + 3)
        with jax.named_scope(f"q#j={j}"):
            q_chunk(j)
        slot(f"q{j}")
    for j in range(n_kv + n_q + 3, n_kv + 2 * n_q):
        start(j)

    n_l = n // 2
    n_h = n_l + 1
    n_a = me // 2 + 1

    def mixed(t):
        ab = jnp.where(t >= n_a, 1, 0)
        return ab, t + ab * (n_l - n_a)

    def mask_step(t, _):
        ab, kb = mixed(t - n_l)
        ab = jnp.where(t < n_l, 1, ab)
        kb = jnp.where(t < n_l, t, kb)
        qp = jnp.where(ab == 1, 2 * n - 1 - me, me)
        sq = seg_s[me, pl.ds(ab, 1), :]
        pos_q = qp * HALF + lax.broadcasted_iota(jnp.int32, (HALF, HALF), 1)
        for h in range(2):
            p = kb * 2 + h
            hi = jnp.where(p >= n, 1, 0)
            d = jnp.where(p >= n, 2 * n - 1 - p, p)
            sk = jnp.transpose(jnp.broadcast_to(seg_s[d, pl.ds(hi, 1), :], (HALF, HALF)))
            pos_k = p * HALF + lax.broadcasted_iota(jnp.int32, (HALF, HALF), 0)
            ok = (sk == sq) & (pos_k <= pos_q)
            b_s[t, h * HALF:(h + 1) * HALF, :] = jnp.where(ok, 0.0, -jnp.inf)
        return 0

    with jax.named_scope("mask"):
        seg_all().wait_recv()
        lax.fori_loop(0, n_l + n_h, mask_step, 0)
    slot("mask")

    rows_g = g_sz * HALF
    scale = LOG2E * DH ** -0.5
    neg = -jnp.inf

    def fold(op, a):
        return op(a.reshape(a.shape[0] // 8, 8, HALF), axis=0)

    def across(op, a):
        return jnp.broadcast_to(op(a, axis=0, keepdims=True), a.shape)

    def heads(s, j):
        return s[:, j * HALF:(j + 1) * HALF]

    def probs(s, m):
        return jnp.exp2((s.reshape(s.shape[0] // 8, 8, HALF) - m[None]) * scale).reshape(s.shape)

    tiles = [range(lo, min(lo + 2, g_sz)) for lo in range(0, g_sz, 2)]

    def span(js):
        return slice(js[0] * HALF, (js[-1] + 1) * HALF)

    def q_of(ab, g, js):
        return q_s[ab, g * g_sz + js[0]:g * g_sz + js[-1] + 1].reshape(len(js) * HALF, DH)

    def scores_low(i, g, js):
        k = kv_s[g, 0:n, 0].reshape(n_l * KB, DH)
        s = lax.dot_general(k, q_of(1, g, js), (((1,), (1,)), ((), ())), preferred_element_type=F32)
        for jj, j in enumerate(js):
            mx = None
            for t in range(n_l):
                sj = heads(s[t * KB:(t + 1) * KB], jj) + b_s[t]
                s_s[i % 2, t, j] = sj
                f = fold(jnp.max, sj)
                mx = f if mx is None else jnp.maximum(mx, f)
            ml_s[g, j] = across(jnp.max, mx)

    def values_low(i, g, js):
        v = jnp.concatenate([kv_s[g, p, 1] for p in range(n)], axis=1)
        ps = []
        for j in js:
            m = ml_s[g, j]
            m = jnp.where(m == neg, 0.0, m)
            cols, tot = [], None
            for t in range(n_l):
                p = probs(s_s[i % 2, t, j], m)
                f = fold(jnp.sum, p)
                tot = f if tot is None else tot + f
                cols.append(p.astype(BF16))
            ll_s[g, j] = tot
            ps.append(jnp.concatenate(cols, axis=0))
        al_s[g, :, span(js)] = jnp.dot(v, jnp.concatenate(ps, axis=1), preferred_element_type=F32)

    order = [0, n_h - 1] + list(range(1, n_h - 1))
    every = range(g_sz)

    def scores_rest(i, g, t):
        ab, kb = (0, 0) if t == 0 else (1, n - 1 - me // 2) if t == n_h - 1 else mixed(t)
        k = kv_s[g, pl.ds(kb * 2, 2), 0].reshape(KB, DH)
        s = lax.dot_general(k, q_of(ab, g, every), (((1,), (1,)), ((), ())), preferred_element_type=F32)
        for j in every:
            sj = heads(s, j) + b_s[n_l + t]
            s_s[i % 2, t, j] = sj
            mx = fold(jnp.max, sj)
            if t == n_h - 1:
                mx = jnp.maximum(mx, ml_s[g, j])
            elif t > 0:
                mx = jnp.maximum(mx, m_s[g % 2, ab, j])
            m_s[g % 2, ab, j] = mx

    def scores_end(i, g):
        for ab in range(2):
            for j in every:
                m_s[g % 2, ab, j] = across(jnp.max, m_s[g % 2, ab, j])

    def values_rest(i, g, t):
        ab, kb = (0, 0) if t == 0 else (1, n - 1 - me // 2) if t == n_h - 1 else mixed(t)
        v = jnp.concatenate([kv_s[g, kb * 2, 1], kv_s[g, kb * 2 + 1, 1]], axis=1)
        ps, corrs = [], []
        for j in every:
            p = probs(s_s[i % 2, t, j], m_s[g % 2, ab, j])
            l = fold(jnp.sum, p)
            if t == n_h - 1:
                corrs.append(jnp.exp2((ml_s[g, j] - m_s[g % 2, 1, j]) * scale))
                l += ll_s[g, j] * corrs[-1]
            elif t > 0:
                l += l_s[ab, j]
            l_s[ab, j] = l
            ps.append(p.astype(BF16))
        a = jnp.dot(v, jnp.concatenate(ps, axis=1), preferred_element_type=F32)
        if t == n_h - 1:
            old = [(al_s[g, :, span([j])].reshape(DH // 8, 8, HALF) * corrs[j][None]).reshape(DH, HALF) for j in every]
            a += jnp.concatenate(old, axis=1)
        elif t > 0:
            a += a_s[ab]
        a_s[ab] = a

    def values_end(i, g):
        for ab in range(2):
            for j in every:
                r = 1.0 / jnp.sum(l_s[ab, j], axis=0, keepdims=True)
                o = jnp.transpose(a_s[ab, :, span([j])] * r).astype(BF16)
                o_s[ab * HALF:(ab + 1) * HALF, (g * g_sz + j) * DH:(g * g_sz + j + 1) * DH] = o

    def parts(i, low, rest, end):
        if i is None:
            return []
        ab, g = units[i]
        if ab == 0:
            return [functools.partial(low, i, g, js) for js in tiles]
        done = [functools.partial(end, i, g)]
        return [functools.partial(rest, i, g, t) for t in order] + done

    def block(i, j):
        if i is not None:
            with jax.named_scope(f"arrived#i={i}"):
                arrived(i)
        with jax.named_scope(f"block#s={i}#v={j}"):
            a = parts(i, scores_low, scores_rest, scores_end)
            b = parts(j, values_low, values_rest, values_end)
            for k in range(max(len(a), len(b))):
                for lst in (a, b):
                    if k < len(lst):
                        lst[k]()

    def project(hf):
        if hf == 0:
            with jax.named_scope("wait_wo"):
                for j in range(n_q):
                    wait(n_kv + n_q + j)
        with jax.named_scope(f"wo#h={hf}"):
            for j in range(n_q):
                o = o_s[:, hf * half_k:(hf + 1) * half_k]
                y = jnp.dot(o, w_s[j, hf * half_k:(hf + 1) * half_k, :], preferred_element_type=F32)
                if hf == 0:
                    y_s[j] = y
                else:
                    y_ref[:, j * NC:(j + 1) * NC] = (y_s[j] + y).astype(BF16)

    last = len(units) - 1
    block(0, None)
    slot("s0")
    for i in range(1, last + 1):
        block(i, i - 1)
        slot(f"s{i}")
        if i == n_kv:
            project(0)
            slot("wo0")
    block(None, last)
    project(1)

    with jax.named_scope("tail"):
        seg_all().wait_send()
        ref = kv_s.at[:, pl.ds(0, 2 * (n - 1))]
        pltpu.make_async_remote_copy(
            src_ref=ref, dst_ref=ref, send_sem=send_sem, recv_sem=rs_sem.at[0],
            device_id={"cp": sib}, device_id_type=MESH).wait_send()


def solution(mesh):
    n = mesh.shape["cp"]

    def local(x, seg, wq, wk, wv, wo):
        lq, d = x.shape
        hq = wq.shape[1] // DH
        hkv = wk.shape[1] // DH
        g_sz = hq // hkv
        n_q = wq.shape[1] // NC
        dma = pltpu.SemaphoreType.DMA
        anyspec = pl.BlockSpec(memory_space=pl.ANY)
        return pl.pallas_call(
            functools.partial(_kernel, n, g_sz),
            out_shape=pltpu.VMEM((lq, wo.shape[1]), BF16),
            in_specs=[anyspec] * 6,
            out_specs=pl.BlockSpec(memory_space=pltpu.VMEM),
            scratch_shapes=[
                pltpu.VMEM((lq, d), BF16),
                pltpu.VMEM((n_q + 2, d, NC), BF16),
                pltpu.VMEM((hkv, 2 * n, 2, HALF, DH), BF16),
                pltpu.VMEM((2, hq, HALF, DH), BF16),
                pltpu.VMEM((lq, hq * DH), BF16),
                pltpu.VMEM((2, n // 2 + 1, g_sz, KB, HALF), F32),
                pltpu.VMEM((n + 1, KB, HALF), F32),
                pltpu.VMEM((2, 2, g_sz, 8, HALF), F32),
                pltpu.VMEM((2, g_sz, 8, HALF), F32),
                pltpu.VMEM((2, DH, g_sz * HALF), F32),
                pltpu.VMEM((hkv, g_sz, 8, HALF), F32),
                pltpu.VMEM((hkv, g_sz, 8, HALF), F32),
                pltpu.VMEM((hkv, DH, g_sz * HALF), F32),
                pltpu.VMEM((n_q, lq, NC), F32),
                pltpu.VMEM((n, 2, HALF), jnp.int32),
                dma, dma((2 * n_q + 2 * hkv,)), dma, dma,
                dma, dma((2 * hkv,)), dma((2 * hkv,)), dma((2 * hkv,)), dma,
            ],
            compiler_params=pltpu.CompilerParams(
                collective_id=0, has_side_effects=True, vmem_limit_bytes=60 * 2 ** 20),
            name="layer",
        )(x, seg.reshape(2, HALF), wq, wk, wv, wo)

    rows = P(("dp", "cp"), None)
    return jax.shard_map(local, mesh=mesh, in_specs=(rows, P(("dp", "cp")), P(), P(), P(), P()), out_specs=rows, check_vma=False)
```

```python
import functools

import jax
import jax.numpy as jnp
from jax import lax
from jax.experimental import pallas as pl
from jax.experimental.pallas import tpu as pltpu
from jax.sharding import PartitionSpec as P

DH = 128
HALF = 128
KB = 256
NC = 512
MESH = pl.DeviceIdType.MESH
F32 = jnp.float32
BF16 = jnp.bfloat16
LOG2E = 1.4426950408889634


def _kernel(n, g_sz, x_hbm, seg_hbm, wq_hbm, wk_hbm, wv_hbm, wo_hbm, y_ref,
            x_s, w_s, kv_s, q_s, s_s, b_s, m_s, l_s, a_s, ml_s, ll_s, al_s, y_s, seg_s,
            x_sem, w_sem, ss_sem, sr_sem, send_sem, rn_sem, rd_sem, rs_sem, loc_sem):
    me = lax.axis_index("cp")
    c, xx, yy = me % 2, (me // 2) % 2, me // 4

    def dev(dy, dx, dc):
        ny = 1 - yy if dy else yy
        nx = 1 - xx if dx else xx
        nc = 1 - c if dc else c
        return ny * 4 + nx * 2 + nc

    d_model = x_s.shape[1]
    n_q = wq_hbm.shape[1] // NC
    n_kv = wk_hbm.shape[1] // DH
    half_k = d_model // 2
    peers = [dev(k // 4, (k // 2) % 2, k % 2) for k in range(n)]
    sib = peers[1]

    def load(i):
        if i < 3:
            slot, rows = (0, pl.ds(i * half_k, half_k)) if i < 2 else (1, pl.ds(0, d_model))
            cols = pl.ds(slot * 2 * DH, 2 * DH)
            return [
                pltpu.make_async_copy(w.at[rows, cols], w_s.at[slot, rows, pl.ds(t * 2 * DH, 2 * DH)], w_sem.at[i + t * 3])
                for t, w in enumerate((wk_hbm, wv_hbm))
            ]
        if i < 3 + n_q:
            j = i - 3
            return [pltpu.make_async_copy(wq_hbm.at[:, pl.ds(j * NC, NC)], w_s.at[2 + j], w_sem.at[i + 3])]
        j = i - 3 - n_q
        return [pltpu.make_async_copy(wo_hbm.at[:, pl.ds(j * NC, NC)], w_s.at[j], w_sem.at[i + 3])]

    def start(i):
        for cp in load(i):
            cp.start()

    def wait(i):
        for cp in load(i):
            cp.wait()

    def x_copy(h):
        cols = pl.ds(h * half_k, half_k)
        return pltpu.make_async_copy(x_hbm.at[:, cols], x_s.at[:, cols], x_sem.at[h])

    seg_cp = pltpu.make_async_copy(seg_hbm, seg_s.at[me], loc_sem)
    x_copy(0).start()
    start(0)
    x_copy(1).start()
    start(1)
    seg_cp.start()

    def seg_copy(k):
        return pltpu.make_async_remote_copy(
            src_ref=seg_s.at[me], dst_ref=seg_s.at[me], send_sem=ss_sem, recv_sem=sr_sem,
            device_id={"cp": peers[k]}, device_id_type=MESH)

    def seg_all():
        ref = seg_s.at[pl.ds(0, n - 1)]
        return pltpu.make_async_remote_copy(
            src_ref=ref, dst_ref=ref, send_sem=ss_sem, recv_sem=sr_sem,
            device_id={"cp": sib}, device_id_type=MESH)

    barrier = pltpu.get_barrier_semaphore()
    for k in range(1, n):
        pl.semaphore_signal(barrier, inc=1, device_id={"cp": peers[k]}, device_id_type=MESH)

    xn, yn, dg = peers[2], peers[4], peers[6]
    first, second = xn * (1 - c) + yn * c, yn * (1 - c) + xn * c

    units = [(ab, g) for g in range(n_kv) for ab in range(2)]

    def chunk(u, src_dev, to, recv):
        ab, g = units[u]
        ref = kv_s.at[g, src_dev if ab == 0 else 2 * n - 1 - src_dev]
        return pltpu.make_async_remote_copy(
            src_ref=ref, dst_ref=ref, send_sem=send_sem, recv_sem=recv.at[u],
            device_id={"cp": to}, device_id_type=MESH)

    def wait_chunks(u, count, recv):
        ref = kv_s.at[u % n_kv, pl.ds(0, count)]
        pltpu.make_async_remote_copy(
            src_ref=ref, dst_ref=ref, send_sem=send_sem, recv_sem=recv.at[u],
            device_id={"cp": sib}, device_id_type=MESH).wait_recv()

    def own(u):
        chunk(u, me, xn, rn_sem).start()
        chunk(u, me, yn, rn_sem).start()
        chunk(u, me, sib, rs_sem).start()

    def forward(u):
        wait_chunks(u, 2, rn_sem)
        chunk(u, first, second, rd_sem).start()
        chunk(u, xn, sib, rs_sem).start()
        chunk(u, yn, sib, rs_sem).start()

    def diag(u):
        wait_chunks(u, 1, rd_sem)
        chunk(u, dg, sib, rs_sem).start()

    def arrived(u):
        wait_chunks(u, 4, rs_sem)

    f, d, o = forward, diag, own
    table = {
        "kv1": ([], [(o, 1)]),
        "q0": ([], [(f, 0), (o, 2)]),
        "q1": ([(o, 1)], []),
        "q2": ([], [(f, 1), (o, 3)]),
        "q3": ([(f, 0), (o, 2)], [(d, 0)]),
        "q4": ([(f, 1)], [(f, 2), (o, 4)]),
        "q5": ([(o, 3), (d, 0)], [(d, 1)]),
        "q6": ([(f, 2), (o, 4)], [(f, 3), (o, 5)]),
        "s0": ([(o, 5), (d, 1)], [(d, 2)]),
        "s1": ([(f, 3), (o, 6), (d, 2)], [(f, 4)]),
        "s2": ([(f, 4), (o, 7), (d, 3)], [(f, 5), (d, 3), (o, 6)]),
        "w0": ([(f, 5), (d, 4)], [(d, 4), (o, 7)]),
        "s3": ([], [(f, 6)]),
        "s4": ([(f, 6), (d, 5)], [(d, 5), (f, 7)]),
        "w1": ([(f, 7), (d, 6)], [(d, 6)]),
        "s6": ([(d, 7)], [(d, 7)]),
    }

    def slot(name):
        early, late = table.get(name, ([], []))
        def run(acts):
            with jax.named_scope(f"slot_{name}"):
                for act, u in acts:
                    act(u)

        if early == late:
            return run(early)
        for cond, acts in ((me < 2, early), (me >= 2, late)):
            if acts:
                pl.when(cond)(functools.partial(run, acts))

    def begin(us):
        with jax.named_scope("barrier"):
            pl.semaphore_wait(barrier, n - 1)
        seg_cp.wait()
        for k in range(1, n):
            seg_copy(k).start()
        for u in us:
            own(u)

    def keep_kv(i, r):
        for gg in range(2):
            for ab in range(2):
                piece = me if ab == 0 else 2 * n - 1 - me
                part = r[ab * HALF:(ab + 1) * HALF]
                kv_s[2 * i + gg, piece, 0] = part[:, gg * DH:(gg + 1) * DH].astype(BF16)
                kv_s[2 * i + gg, piece, 1] = jnp.transpose(part[:, (2 + gg) * DH:(3 + gg) * DH]).astype(BF16)

    with jax.named_scope("wait_x0"):
        x_copy(0).wait()
        wait(0)
        start(2)
    with jax.named_scope("kv0a"):
        y_s[0] = jnp.dot(x_s[:, :half_k], w_s[0, :half_k], preferred_element_type=F32)
    with jax.named_scope("wait_x1"):
        x_copy(1).wait()
        wait(1)
        start(3)
    with jax.named_scope("kv0b"):
        keep_kv(0, y_s[0] + jnp.dot(x_s[:, half_k:], w_s[0, half_k:], preferred_element_type=F32))
    pl.when(me >= 2)(functools.partial(begin, [0]))
    with jax.named_scope("wait_kv1"):
        wait(2)
        start(4)
        start(5)
    with jax.named_scope("kv1"):
        keep_kv(1, jnp.dot(x_s[...], w_s[1], preferred_element_type=F32))
    pl.when(me < 2)(functools.partial(begin, [0]))
    slot("kv1")

    n_l = n // 2
    n_h = n_l + 1
    n_a = me // 2 + 1

    def mixed(t):
        ab = jnp.where(t >= n_a, 1, 0)
        return ab, t + ab * (n_l - n_a)

    def mask_step(t):
        ab, kb = mixed(t - n_l)
        ab = jnp.where(t < n_l, 1, ab)
        kb = jnp.where(t < n_l, t, kb)
        qp = jnp.where(ab == 1, 2 * n - 1 - me, me)
        sq = seg_s[me, pl.ds(ab, 1), :]
        pos_q = qp * HALF + lax.broadcasted_iota(jnp.int32, (HALF, HALF), 1)
        for h in range(2):
            p = kb * 2 + h
            hi = jnp.where(p >= n, 1, 0)
            d = jnp.where(p >= n, 2 * n - 1 - p, p)
            sk = jnp.transpose(jnp.broadcast_to(seg_s[d, pl.ds(hi, 1), :], (HALF, HALF)))
            pos_k = p * HALF + lax.broadcasted_iota(jnp.int32, (HALF, HALF), 0)
            ok = (sk == sq) & (pos_k <= pos_q)
            b_s[t, h * HALF:(h + 1) * HALF, :] = jnp.where(ok, 0.0, -jnp.inf)

    def q_chunk(j):
        r = jnp.dot(x_s[...], w_s[2 + j], preferred_element_type=F32).astype(BF16)
        for hh in range(NC // DH):
            for ab in range(2):
                q_s[ab, j * (NC // DH) + hh] = r[ab * HALF:(ab + 1) * HALF, hh * DH:(hh + 1) * DH]

    nexts = [[6 + j] for j in range(n_q - 2)] + [[4 + n_q, 5 + n_q], [6 + n_q, 7 + n_q]]
    for j in range(n_q):
        with jax.named_scope(f"wait_q#j={j}"):
            wait(3 + j)
            for i in nexts[j]:
                start(i)
            if j == n_q - 2:
                seg_all().wait_recv()
        with jax.named_scope(f"q#j={j}"):
            if j >= n_q - 2:
                for t in range(n_l + n_h):
                    if (t < n_l) == (j == n_q - 2):
                        mask_step(t)
            q_chunk(j)
        slot(f"q{j}")
    for i in range(8 + n_q, 3 + 2 * n_q):
        start(i)

    o_s = x_s
    rows_g = g_sz * HALF
    scale = LOG2E * DH ** -0.5
    neg = -jnp.inf

    def fold(op, a):
        return op(a.reshape(a.shape[0] // 8, 8, HALF), axis=0)

    def across(op, a):
        return jnp.broadcast_to(op(a, axis=0, keepdims=True), a.shape)

    def heads(s, j):
        return s[:, j * HALF:(j + 1) * HALF]

    def probs(s, m):
        return jnp.exp2((s.reshape(s.shape[0] // 8, 8, HALF) - m[None]) * scale).reshape(s.shape)

    tiles = [range(lo, min(lo + 2, g_sz)) for lo in range(0, g_sz, 2)]

    def span(js):
        return slice(js[0] * HALF, (js[-1] + 1) * HALF)

    def q_of(ab, g, js):
        return q_s[ab, g * g_sz + js[0]:g * g_sz + js[-1] + 1].reshape(len(js) * HALF, DH)

    def scores_low(i, g, js):
        k = kv_s[g, 0:n, 0].reshape(n_l * KB, DH)
        s = lax.dot_general(k, q_of(1, g, js), (((1,), (1,)), ((), ())), preferred_element_type=F32)
        for jj, j in enumerate(js):
            mx = None
            for t in range(n_l):
                sj = heads(s[t * KB:(t + 1) * KB], jj) + b_s[t]
                s_s[i % 2, t, j] = sj
                f = fold(jnp.max, sj)
                mx = f if mx is None else jnp.maximum(mx, f)
            ml_s[g, j] = across(jnp.max, mx)

    def values_low(i, g, js):
        v = jnp.concatenate([kv_s[g, p, 1] for p in range(n)], axis=1)
        ps = []
        for j in js:
            m = ml_s[g, j]
            m = jnp.where(m == neg, 0.0, m)
            cols, tot = [], None
            for t in range(n_l):
                p = probs(s_s[i % 2, t, j], m)
                f = fold(jnp.sum, p)
                tot = f if tot is None else tot + f
                cols.append(p.astype(BF16))
            ll_s[g, j] = tot
            ps.append(jnp.concatenate(cols, axis=0))
        al_s[g, :, span(js)] = jnp.dot(v, jnp.concatenate(ps, axis=1), preferred_element_type=F32)

    order = [0, n_h - 1] + list(range(1, n_h - 1))
    every = range(g_sz)

    def scores_rest(i, g, t):
        ab, kb = (0, 0) if t == 0 else (1, n - 1 - me // 2) if t == n_h - 1 else mixed(t)
        k = kv_s[g, pl.ds(kb * 2, 2), 0].reshape(KB, DH)
        s = lax.dot_general(k, q_of(ab, g, every), (((1,), (1,)), ((), ())), preferred_element_type=F32)
        for j in every:
            sj = heads(s, j) + b_s[n_l + t]
            s_s[i % 2, t, j] = sj
            mx = fold(jnp.max, sj)
            if t == n_h - 1:
                mx = jnp.maximum(mx, ml_s[g, j])
            elif t > 0:
                mx = jnp.maximum(mx, m_s[g % 2, ab, j])
            m_s[g % 2, ab, j] = mx

    def scores_end(i, g):
        for ab in range(2):
            for j in every:
                m_s[g % 2, ab, j] = across(jnp.max, m_s[g % 2, ab, j])

    def values_rest(i, g, t):
        ab, kb = (0, 0) if t == 0 else (1, n - 1 - me // 2) if t == n_h - 1 else mixed(t)
        v = jnp.concatenate([kv_s[g, kb * 2, 1], kv_s[g, kb * 2 + 1, 1]], axis=1)
        ps, corrs = [], []
        for j in every:
            p = probs(s_s[i % 2, t, j], m_s[g % 2, ab, j])
            l = fold(jnp.sum, p)
            if t == n_h - 1:
                corrs.append(jnp.exp2((ml_s[g, j] - m_s[g % 2, 1, j]) * scale))
                l += ll_s[g, j] * corrs[-1]
            elif t > 0:
                l += l_s[ab, j]
            l_s[ab, j] = l
            ps.append(p.astype(BF16))
        a = jnp.dot(v, jnp.concatenate(ps, axis=1), preferred_element_type=F32)
        if t == n_h - 1:
            old = [(al_s[g, :, span([j])].reshape(DH // 8, 8, HALF) * corrs[j][None]).reshape(DH, HALF) for j in every]
            a += jnp.concatenate(old, axis=1)
        elif t > 0:
            a += a_s[ab]
        a_s[ab] = a

    def values_end(i, g):
        for ab in range(2):
            for j in every:
                r = 1.0 / jnp.sum(l_s[ab, j], axis=0, keepdims=True)
                o = jnp.transpose(a_s[ab, :, span([j])] * r).astype(BF16)
                o_s[ab * HALF:(ab + 1) * HALF, (g * g_sz + j) * DH:(g * g_sz + j + 1) * DH] = o

    def parts(i, low, rest, end):
        if i is None:
            return []
        ab, g = units[i]
        if ab == 0:
            return [functools.partial(low, i, g, js) for js in tiles]
        done = [functools.partial(end, i, g)]
        return [functools.partial(rest, i, g, t) for t in order] + done

    def block(i, j):
        if i is not None:
            with jax.named_scope(f"arrived#i={i}"):
                arrived(i)
        with jax.named_scope(f"block#s={i}#v={j}"):
            a = parts(i, scores_low, scores_rest, scores_end)
            b = parts(j, values_low, values_rest, values_end)
            for k in range(max(len(a), len(b))):
                for lst in (a, b):
                    if k < len(lst):
                        lst[k]()

    cuts = [min(g * g_sz * DH // KB * KB, d_model) for g in range(n_kv)] + [d_model]

    def project(g):
        if g == 0:
            with jax.named_scope("wait_wo"):
                for j in range(n_q):
                    wait(3 + n_q + j)
        rows = slice(cuts[g], cuts[g + 1])
        with jax.named_scope(f"wo#g={g}"):
            for j in range(n_q):
                y = jnp.dot(o_s[:, rows], w_s[j, rows, :], preferred_element_type=F32)
                if g > 0:
                    y += y_s[j]
                if g < n_kv - 1:
                    y_s[j] = y
                else:
                    y_ref[:, j * NC:(j + 1) * NC] = y.astype(BF16)

    block(0, None)
    slot("s0")
    for i in range(1, len(units)):
        block(i, i - 1)
        slot(f"s{i}")
        if i % 2 == 0:
            project(i // 2 - 1)
            slot(f"w{i // 2 - 1}")
    block(None, len(units) - 1)
    project(n_kv - 1)

    with jax.named_scope("tail"):
        seg_all().wait_send()
        ref = kv_s.at[:, pl.ds(0, 2 * (n - 1))]
        pltpu.make_async_remote_copy(
            src_ref=ref, dst_ref=ref, send_sem=send_sem, recv_sem=rs_sem.at[0],
            device_id={"cp": sib}, device_id_type=MESH).wait_send()


def solution(mesh):
    n = mesh.shape["cp"]

    def local(x, seg, wq, wk, wv, wo):
        lq, d = x.shape
        hq = wq.shape[1] // DH
        hkv = wk.shape[1] // DH
        g_sz = hq // hkv
        n_q = wq.shape[1] // NC
        dma = pltpu.SemaphoreType.DMA
        anyspec = pl.BlockSpec(memory_space=pl.ANY)
        return pl.pallas_call(
            functools.partial(_kernel, n, g_sz),
            out_shape=pltpu.VMEM((lq, wo.shape[1]), BF16),
            in_specs=[anyspec] * 6,
            out_specs=pl.BlockSpec(memory_space=pltpu.VMEM),
            scratch_shapes=[
                pltpu.VMEM((lq, d), BF16),
                pltpu.VMEM((n_q + 2, d, NC), BF16),
                pltpu.VMEM((hkv, 2 * n, 2, HALF, DH), BF16),
                pltpu.VMEM((2, hq, HALF, DH), BF16),
                pltpu.VMEM((2, n // 2 + 1, g_sz, KB, HALF), F32),
                pltpu.VMEM((n + 1, KB, HALF), F32),
                pltpu.VMEM((2, 2, g_sz, 8, HALF), F32),
                pltpu.VMEM((2, g_sz, 8, HALF), F32),
                pltpu.VMEM((2, DH, g_sz * HALF), F32),
                pltpu.VMEM((hkv, g_sz, 8, HALF), F32),
                pltpu.VMEM((hkv, g_sz, 8, HALF), F32),
                pltpu.VMEM((hkv, DH, g_sz * HALF), F32),
                pltpu.VMEM((n_q, lq, NC), F32),
                pltpu.VMEM((n, 2, HALF), jnp.int32),
                dma((2,)), dma((2 * n_q + 6,)), dma, dma,
                dma, dma((2 * hkv,)), dma((2 * hkv,)), dma((2 * hkv,)), dma,
            ],
            compiler_params=pltpu.CompilerParams(
                collective_id=0, has_side_effects=True, vmem_limit_bytes=60 * 2 ** 20),
            name="layer",
        )(x, seg.reshape(2, HALF), wq, wk, wv, wo)

    rows = P(("dp", "cp"), None)
    return jax.shard_map(local, mesh=mesh, in_specs=(rows, P(("dp", "cp")), P(), P(), P(), P()), out_specs=rows, check_vma=False)
```

```python
import functools

import jax
import jax.numpy as jnp
from jax import lax
from jax.experimental import pallas as pl
from jax.experimental.pallas import tpu as pltpu
from jax.sharding import PartitionSpec as P

DH = 128
HALF = 128
KB = 256
NC = 512
MESH = pl.DeviceIdType.MESH
F32 = jnp.float32
BF16 = jnp.bfloat16
LOG2E = 1.4426950408889634


def _kernel(n, g_sz, x_hbm, seg_hbm, wq_hbm, wk_hbm, wv_hbm, wo_hbm, y_ref,
            x_s, w_s, kv_s, q_s, s_s, b_s, m_s, l_s, a_s, ml_s, ll_s, al_s, y_s, seg_s,
            x_sem, w_sem, ss_sem, sr_sem, send_sem, rn_sem, rd_sem, rs_sem, loc_sem):
    me = lax.axis_index("cp")
    c, xx, yy = me % 2, (me // 2) % 2, me // 4

    def dev(dy, dx, dc):
        ny = 1 - yy if dy else yy
        nx = 1 - xx if dx else xx
        nc = 1 - c if dc else c
        return ny * 4 + nx * 2 + nc

    d_model = x_s.shape[1]
    n_q = wq_hbm.shape[1] // NC
    n_kv = wk_hbm.shape[1] // DH
    half_k = d_model // 2
    peers = [dev(k // 4, (k // 2) % 2, k % 2) for k in range(n)]
    sib = peers[1]

    def load(i):
        if i < 3:
            slot, rows = (0, pl.ds(i * half_k, half_k)) if i < 2 else (1, pl.ds(0, d_model))
            cols = pl.ds(slot * 2 * DH, 2 * DH)
            return [
                pltpu.make_async_copy(w.at[rows, cols], w_s.at[slot, rows, pl.ds(t * 2 * DH, 2 * DH)], w_sem.at[i + t * 3])
                for t, w in enumerate((wk_hbm, wv_hbm))
            ]
        if i < 3 + n_q:
            j = i - 3
            return [pltpu.make_async_copy(wq_hbm.at[:, pl.ds(j * NC, NC)], w_s.at[2 + j], w_sem.at[i + 3])]
        j = i - 3 - n_q
        return [pltpu.make_async_copy(wo_hbm.at[:, pl.ds(j * NC, NC)], w_s.at[j], w_sem.at[i + 3])]

    def start(i):
        for cp in load(i):
            cp.start()

    def wait(i):
        for cp in load(i):
            cp.wait()

    def x_copy(h):
        cols = pl.ds(h * half_k, half_k)
        return pltpu.make_async_copy(x_hbm.at[:, cols], x_s.at[:, cols], x_sem.at[h])

    seg_cp = pltpu.make_async_copy(seg_hbm, seg_s.at[me], loc_sem)
    x_copy(0).start()
    start(0)
    x_copy(1).start()
    start(1)
    seg_cp.start()

    def seg_copy(k):
        return pltpu.make_async_remote_copy(
            src_ref=seg_s.at[me], dst_ref=seg_s.at[me], send_sem=ss_sem, recv_sem=sr_sem,
            device_id={"cp": peers[k]}, device_id_type=MESH)

    def seg_all():
        ref = seg_s.at[pl.ds(0, n - 1)]
        return pltpu.make_async_remote_copy(
            src_ref=ref, dst_ref=ref, send_sem=ss_sem, recv_sem=sr_sem,
            device_id={"cp": sib}, device_id_type=MESH)

    barrier = pltpu.get_barrier_semaphore()
    for k in range(1, n):
        pl.semaphore_signal(barrier, inc=1, device_id={"cp": peers[k]}, device_id_type=MESH)

    xn, yn, dg = peers[2], peers[4], peers[6]
    first, second = xn * (1 - c) + yn * c, yn * (1 - c) + xn * c

    units = [(ab, g) for g in range(n_kv) for ab in range(2)]

    def chunk(u, src_dev, to, recv):
        ab, g = units[u]
        ref = kv_s.at[g, src_dev if ab == 0 else 2 * n - 1 - src_dev]
        return pltpu.make_async_remote_copy(
            src_ref=ref, dst_ref=ref, send_sem=send_sem, recv_sem=recv.at[u],
            device_id={"cp": to}, device_id_type=MESH)

    def wait_chunks(u, count, recv):
        ref = kv_s.at[u % n_kv, pl.ds(0, count)]
        pltpu.make_async_remote_copy(
            src_ref=ref, dst_ref=ref, send_sem=send_sem, recv_sem=recv.at[u],
            device_id={"cp": sib}, device_id_type=MESH).wait_recv()

    def own(u):
        chunk(u, me, xn, rn_sem).start()
        chunk(u, me, yn, rn_sem).start()
        chunk(u, me, sib, rs_sem).start()

    def forward(u):
        wait_chunks(u, 2, rn_sem)
        chunk(u, first, second, rd_sem).start()
        chunk(u, xn, sib, rs_sem).start()
        chunk(u, yn, sib, rs_sem).start()

    def diag(u):
        wait_chunks(u, 1, rd_sem)
        chunk(u, dg, sib, rs_sem).start()

    def arrived(u):
        wait_chunks(u, 4, rs_sem)

    f, d, o = forward, diag, own
    table = {
        "kv1": ([], [(o, 1)]),
        "q0": ([], [(f, 0), (o, 2)]),
        "q1": ([(o, 1)], []),
        "q2": ([], [(f, 1), (o, 3)]),
        "q3": ([(f, 0), (o, 2)], [(d, 0)]),
        "q4": ([(f, 1)], [(f, 2)]),
        "q5": ([(o, 3), (d, 0)], [(o, 4), (d, 1)]),
        "q6": ([(f, 2), (o, 4)], [(f, 3), (o, 5)]),
        "s0": ([(o, 5), (d, 1)], [(d, 2)]),
        "s1": ([(f, 3), (o, 6), (d, 2)], [(f, 4)]),
        "s2": ([(f, 4), (o, 7), (d, 3)], [(f, 5), (d, 3), (o, 6)]),
        "w0": ([(f, 5), (d, 4)], [(d, 4), (o, 7)]),
        "s3": ([], [(f, 6)]),
        "s4": ([(f, 6), (d, 5)], [(d, 5), (f, 7)]),
        "w1": ([(f, 7), (d, 6)], [(d, 6)]),
        "s6": ([(d, 7)], [(d, 7)]),
    }

    def slot(name):
        early, late = table.get(name, ([], []))
        def run(acts):
            with jax.named_scope(f"slot_{name}"):
                for act, u in acts:
                    act(u)

        if early == late:
            return run(early)
        for cond, acts in ((me < 2, early), (me >= 2, late)):
            if acts:
                pl.when(cond)(functools.partial(run, acts))

    def begin(us):
        with jax.named_scope("barrier"):
            pl.semaphore_wait(barrier, n - 1)
        seg_cp.wait()
        for k in range(1, n):
            seg_copy(k).start()
        for u in us:
            own(u)

    def keep_kv(i, r):
        for gg in range(2):
            for ab in range(2):
                piece = me if ab == 0 else 2 * n - 1 - me
                part = r[ab * HALF:(ab + 1) * HALF]
                kv_s[2 * i + gg, piece, 0] = part[:, gg * DH:(gg + 1) * DH].astype(BF16)
                kv_s[2 * i + gg, piece, 1] = jnp.transpose(part[:, (2 + gg) * DH:(3 + gg) * DH]).astype(BF16)

    with jax.named_scope("wait_x0"):
        x_copy(0).wait()
        wait(0)
        start(2)
    with jax.named_scope("kv0a"):
        y_s[0] = jnp.dot(x_s[:, :half_k], w_s[0, :half_k], preferred_element_type=F32)
    with jax.named_scope("wait_x1"):
        x_copy(1).wait()
        wait(1)
        start(3)
    with jax.named_scope("kv0b"):
        keep_kv(0, y_s[0] + jnp.dot(x_s[:, half_k:], w_s[0, half_k:], preferred_element_type=F32))
    pl.when(me >= 2)(functools.partial(begin, [0]))
    with jax.named_scope("wait_kv1"):
        wait(2)
        start(4)
        start(5)
    with jax.named_scope("kv1"):
        keep_kv(1, jnp.dot(x_s[...], w_s[1], preferred_element_type=F32))
    pl.when(me < 2)(functools.partial(begin, [0]))
    slot("kv1")

    n_l = n // 2
    n_h = n_l + 1
    n_a = me // 2 + 1

    def mixed(t):
        ab = jnp.where(t >= n_a, 1, 0)
        return ab, t + ab * (n_l - n_a)

    def mask_step(t):
        ab, kb = mixed(t - n_l)
        ab = jnp.where(t < n_l, 1, ab)
        kb = jnp.where(t < n_l, t, kb)
        qp = jnp.where(ab == 1, 2 * n - 1 - me, me)
        sq = seg_s[me, pl.ds(ab, 1), :]
        pos_q = qp * HALF + lax.broadcasted_iota(jnp.int32, (HALF, HALF), 1)
        for h in range(2):
            p = kb * 2 + h
            hi = jnp.where(p >= n, 1, 0)
            d = jnp.where(p >= n, 2 * n - 1 - p, p)
            sk = jnp.transpose(jnp.broadcast_to(seg_s[d, pl.ds(hi, 1), :], (HALF, HALF)))
            pos_k = p * HALF + lax.broadcasted_iota(jnp.int32, (HALF, HALF), 0)
            ok = (sk == sq) & (pos_k <= pos_q)
            b_s[t, h * HALF:(h + 1) * HALF, :] = jnp.where(ok, 0.0, -jnp.inf)

    def q_chunk(j):
        r = jnp.dot(x_s[...], w_s[2 + j], preferred_element_type=F32).astype(BF16)
        for hh in range(NC // DH):
            for ab in range(2):
                q_s[ab, j * (NC // DH) + hh] = r[ab * HALF:(ab + 1) * HALF, hh * DH:(hh + 1) * DH]

    nexts = [[6 + j] for j in range(n_q - 2)] + [[4 + n_q, 5 + n_q], [6 + n_q, 7 + n_q]]
    for j in range(n_q):
        with jax.named_scope(f"wait_q#j={j}"):
            wait(3 + j)
            for i in nexts[j]:
                start(i)
            if j == n_q - 2:
                seg_all().wait_recv()
        with jax.named_scope(f"q#j={j}"):
            if j >= n_q - 2:
                for t in range(n_l + n_h):
                    if (t < n_l) == (j == n_q - 2):
                        mask_step(t)
            q_chunk(j)
        slot(f"q{j}")
    for i in range(8 + n_q, 3 + 2 * n_q):
        start(i)

    o_s = x_s
    rows_g = g_sz * HALF
    scale = LOG2E * DH ** -0.5
    neg = -jnp.inf

    def fold(op, a):
        return op(a.reshape(a.shape[0] // 8, 8, HALF), axis=0)

    def across(op, a):
        return jnp.broadcast_to(op(a, axis=0, keepdims=True), a.shape)

    def heads(s, j):
        return s[:, j * HALF:(j + 1) * HALF]

    def probs(s, m):
        return jnp.exp2((s.reshape(s.shape[0] // 8, 8, HALF) - m[None]) * scale).reshape(s.shape)

    tiles = [range(lo, min(lo + 2, g_sz)) for lo in range(0, g_sz, 2)]

    def span(js):
        return slice(js[0] * HALF, (js[-1] + 1) * HALF)

    def q_of(ab, g, js):
        return q_s[ab, g * g_sz + js[0]:g * g_sz + js[-1] + 1].reshape(len(js) * HALF, DH)

    def scores_low(i, g, js):
        k = kv_s[g, 0:n, 0].reshape(n_l * KB, DH)
        s = lax.dot_general(k, q_of(1, g, js), (((1,), (1,)), ((), ())), preferred_element_type=F32)
        for jj, j in enumerate(js):
            mx = None
            for t in range(n_l):
                sj = heads(s[t * KB:(t + 1) * KB], jj) + b_s[t]
                s_s[i % 2, t, j] = sj
                f = fold(jnp.max, sj)
                mx = f if mx is None else jnp.maximum(mx, f)
            ml_s[g, j] = across(jnp.max, mx)

    def values_low(i, g, js):
        v = jnp.concatenate([kv_s[g, p, 1] for p in range(n)], axis=1)
        ps = []
        for j in js:
            m = ml_s[g, j]
            m = jnp.where(m == neg, 0.0, m)
            cols, tot = [], None
            for t in range(n_l):
                p = probs(s_s[i % 2, t, j], m)
                f = fold(jnp.sum, p)
                tot = f if tot is None else tot + f
                cols.append(p.astype(BF16))
            ll_s[g, j] = tot
            ps.append(jnp.concatenate(cols, axis=0))
        al_s[g, :, span(js)] = jnp.dot(v, jnp.concatenate(ps, axis=1), preferred_element_type=F32)

    order = [0, n_h - 1] + list(range(1, n_h - 1))
    every = range(g_sz)

    def scores_rest(i, g, t):
        ab, kb = (0, 0) if t == 0 else (1, n - 1 - me // 2) if t == n_h - 1 else mixed(t)
        k = kv_s[g, pl.ds(kb * 2, 2), 0].reshape(KB, DH)
        s = lax.dot_general(k, q_of(ab, g, every), (((1,), (1,)), ((), ())), preferred_element_type=F32)
        for j in every:
            sj = heads(s, j) + b_s[n_l + t]
            s_s[i % 2, t, j] = sj
            mx = fold(jnp.max, sj)
            if t == n_h - 1:
                mx = jnp.maximum(mx, ml_s[g, j])
            elif t > 0:
                mx = jnp.maximum(mx, m_s[g % 2, ab, j])
            m_s[g % 2, ab, j] = mx

    def scores_end(i, g):
        for ab in range(2):
            for j in every:
                m_s[g % 2, ab, j] = across(jnp.max, m_s[g % 2, ab, j])

    def values_rest(i, g, t):
        ab, kb = (0, 0) if t == 0 else (1, n - 1 - me // 2) if t == n_h - 1 else mixed(t)
        v = jnp.concatenate([kv_s[g, kb * 2, 1], kv_s[g, kb * 2 + 1, 1]], axis=1)
        ps, corrs = [], []
        for j in every:
            p = probs(s_s[i % 2, t, j], m_s[g % 2, ab, j])
            l = fold(jnp.sum, p)
            if t == n_h - 1:
                corrs.append(jnp.exp2((ml_s[g, j] - m_s[g % 2, 1, j]) * scale))
                l += ll_s[g, j] * corrs[-1]
            elif t > 0:
                l += l_s[ab, j]
            l_s[ab, j] = l
            ps.append(p.astype(BF16))
        a = jnp.dot(v, jnp.concatenate(ps, axis=1), preferred_element_type=F32)
        if t == n_h - 1:
            old = [(al_s[g, :, span([j])].reshape(DH // 8, 8, HALF) * corrs[j][None]).reshape(DH, HALF) for j in every]
            a += jnp.concatenate(old, axis=1)
        elif t > 0:
            a += a_s[ab]
        a_s[ab] = a

    def values_end(i, g):
        for ab in range(2):
            for j in every:
                r = 1.0 / jnp.sum(l_s[ab, j], axis=0, keepdims=True)
                o = jnp.transpose(a_s[ab, :, span([j])] * r).astype(BF16)
                o_s[ab * HALF:(ab + 1) * HALF, (g * g_sz + j) * DH:(g * g_sz + j + 1) * DH] = o

    def parts(i, low, rest, end):
        if i is None:
            return []
        ab, g = units[i]
        if ab == 0:
            return [functools.partial(low, i, g, js) for js in tiles]
        done = [functools.partial(end, i, g)]
        return [functools.partial(rest, i, g, t) for t in order] + done

    def block(i, j):
        if i is not None:
            with jax.named_scope(f"arrived#i={i}"):
                arrived(i)
        with jax.named_scope(f"block#s={i}#v={j}"):
            a = parts(i, scores_low, scores_rest, scores_end)
            b = parts(j, values_low, values_rest, values_end)
            for k in range(max(len(a), len(b))):
                for lst in (a, b):
                    if k < len(lst):
                        lst[k]()

    cuts = [min(g * g_sz * DH // KB * KB, d_model) for g in range(n_kv)] + [d_model]

    def project(g):
        if g == 0:
            with jax.named_scope("wait_wo"):
                for j in range(n_q):
                    wait(3 + n_q + j)
        rows = slice(cuts[g], cuts[g + 1])
        with jax.named_scope(f"wo#g={g}"):
            for j in range(n_q):
                y = jnp.dot(o_s[:, rows], w_s[j, rows, :], preferred_element_type=F32)
                if g > 0:
                    y += y_s[j]
                if g < n_kv - 1:
                    y_s[j] = y
                else:
                    y_ref[:, j * NC:(j + 1) * NC] = y.astype(BF16)

    block(0, None)
    slot("s0")
    for i in range(1, len(units)):
        block(i, i - 1)
        slot(f"s{i}")
        if i % 2 == 0:
            project(i // 2 - 1)
            slot(f"w{i // 2 - 1}")
    block(None, len(units) - 1)
    project(n_kv - 1)

    with jax.named_scope("tail"):
        seg_all().wait_send()
        ref = kv_s.at[:, pl.ds(0, 2 * (n - 1))]
        pltpu.make_async_remote_copy(
            src_ref=ref, dst_ref=ref, send_sem=send_sem, recv_sem=rs_sem.at[0],
            device_id={"cp": sib}, device_id_type=MESH).wait_send()


def solution(mesh):
    n = mesh.shape["cp"]

    def local(x, seg, wq, wk, wv, wo):
        lq, d = x.shape
        hq = wq.shape[1] // DH
        hkv = wk.shape[1] // DH
        g_sz = hq // hkv
        n_q = wq.shape[1] // NC
        dma = pltpu.SemaphoreType.DMA
        anyspec = pl.BlockSpec(memory_space=pl.ANY)
        return pl.pallas_call(
            functools.partial(_kernel, n, g_sz),
            out_shape=pltpu.VMEM((lq, wo.shape[1]), BF16),
            in_specs=[anyspec] * 6,
            out_specs=pl.BlockSpec(memory_space=pltpu.VMEM),
            scratch_shapes=[
                pltpu.VMEM((lq, d), BF16),
                pltpu.VMEM((n_q + 2, d, NC), BF16),
                pltpu.VMEM((hkv, 2 * n, 2, HALF, DH), BF16),
                pltpu.VMEM((2, hq, HALF, DH), BF16),
                pltpu.VMEM((2, n // 2 + 1, g_sz, KB, HALF), F32),
                pltpu.VMEM((n + 1, KB, HALF), F32),
                pltpu.VMEM((2, 2, g_sz, 8, HALF), F32),
                pltpu.VMEM((2, g_sz, 8, HALF), F32),
                pltpu.VMEM((2, DH, g_sz * HALF), F32),
                pltpu.VMEM((hkv, g_sz, 8, HALF), F32),
                pltpu.VMEM((hkv, g_sz, 8, HALF), F32),
                pltpu.VMEM((hkv, DH, g_sz * HALF), F32),
                pltpu.VMEM((n_q, lq, NC), F32),
                pltpu.VMEM((n, 2, HALF), jnp.int32),
                dma((2,)), dma((2 * n_q + 6,)), dma, dma,
                dma, dma((2 * hkv,)), dma((2 * hkv,)), dma((2 * hkv,)), dma,
            ],
            compiler_params=pltpu.CompilerParams(
                collective_id=0, has_side_effects=True, vmem_limit_bytes=60 * 2 ** 20),
            name="layer",
        )(x, seg.reshape(2, HALF), wq, wk, wv, wo)

    rows = P(("dp", "cp"), None)
    return jax.shard_map(local, mesh=mesh, in_specs=(rows, P(("dp", "cp")), P(), P(), P(), P()), out_specs=rows, check_vma=False)
```

```python
import functools

import jax
import jax.numpy as jnp
from jax import lax
from jax.experimental import pallas as pl
from jax.experimental.pallas import tpu as pltpu
from jax.sharding import PartitionSpec as P

DH = 128
HALF = 128
KB = 256
NC = 512
MESH = pl.DeviceIdType.MESH
F32 = jnp.float32
BF16 = jnp.bfloat16
LOG2E = 1.4426950408889634


def _kernel(n, g_sz, x_hbm, seg_hbm, wq_hbm, wk_hbm, wv_hbm, wo_hbm, y_ref,
            x_s, w_s, kv_s, q_s, s_s, b_s, m_s, l_s, a_s, ml_s, ll_s, al_s, y_s, seg_s,
            x_sem, w_sem, ss_sem, sr_sem, send_sem, rn_sem, rd_sem, rs_sem, loc_sem):
    me = lax.axis_index("cp")
    c, xx, yy = me % 2, (me // 2) % 2, me // 4

    def dev(dy, dx, dc):
        ny = 1 - yy if dy else yy
        nx = 1 - xx if dx else xx
        nc = 1 - c if dc else c
        return ny * 4 + nx * 2 + nc

    d_model = x_s.shape[1]
    n_q = wq_hbm.shape[1] // NC
    n_kv = wk_hbm.shape[1] // DH
    half_k = d_model // 2
    peers = [dev(k // 4, (k // 2) % 2, k % 2) for k in range(n)]
    sib = peers[1]

    def load(i):
        if i < 3:
            slot, rows = (0, pl.ds(i * half_k, half_k)) if i < 2 else (1, pl.ds(0, d_model))
            cols = pl.ds(slot * 2 * DH, 2 * DH)
            return [
                pltpu.make_async_copy(w.at[rows, cols], w_s.at[slot, rows, pl.ds(t * 2 * DH, 2 * DH)], w_sem.at[i + t * 3])
                for t, w in enumerate((wk_hbm, wv_hbm))
            ]
        if i < 3 + n_q:
            j = i - 3
            return [pltpu.make_async_copy(wq_hbm.at[:, pl.ds(j * NC, NC)], w_s.at[2 + j], w_sem.at[i + 3])]
        j = i - 3 - n_q
        return [pltpu.make_async_copy(wo_hbm.at[:, pl.ds(j * NC, NC)], w_s.at[j], w_sem.at[i + 3])]

    def start(i):
        for cp in load(i):
            cp.start()

    def wait(i):
        for cp in load(i):
            cp.wait()

    def x_copy(h):
        cols = pl.ds(h * half_k, half_k)
        return pltpu.make_async_copy(x_hbm.at[:, cols], x_s.at[:, cols], x_sem.at[h])

    seg_cp = pltpu.make_async_copy(seg_hbm, seg_s.at[me], loc_sem)
    x_copy(0).start()
    start(0)
    x_copy(1).start()
    start(1)
    seg_cp.start()

    def seg_copy(k):
        return pltpu.make_async_remote_copy(
            src_ref=seg_s.at[me], dst_ref=seg_s.at[me], send_sem=ss_sem, recv_sem=sr_sem,
            device_id={"cp": peers[k]}, device_id_type=MESH)

    def seg_all():
        ref = seg_s.at[pl.ds(0, n - 1)]
        return pltpu.make_async_remote_copy(
            src_ref=ref, dst_ref=ref, send_sem=ss_sem, recv_sem=sr_sem,
            device_id={"cp": sib}, device_id_type=MESH)

    barrier = pltpu.get_barrier_semaphore()
    for k in range(1, n):
        pl.semaphore_signal(barrier, inc=1, device_id={"cp": peers[k]}, device_id_type=MESH)

    xn, yn, dg = peers[2], peers[4], peers[6]
    first, second = xn * (1 - c) + yn * c, yn * (1 - c) + xn * c

    units = [(ab, g) for g in range(n_kv) for ab in range(2)]

    def chunk(u, src_dev, to, recv):
        ab, g = units[u]
        ref = kv_s.at[g, src_dev if ab == 0 else 2 * n - 1 - src_dev]
        return pltpu.make_async_remote_copy(
            src_ref=ref, dst_ref=ref, send_sem=send_sem, recv_sem=recv.at[u],
            device_id={"cp": to}, device_id_type=MESH)

    def wait_chunks(u, count, recv):
        ref = kv_s.at[u % n_kv, pl.ds(0, count)]
        pltpu.make_async_remote_copy(
            src_ref=ref, dst_ref=ref, send_sem=send_sem, recv_sem=recv.at[u],
            device_id={"cp": sib}, device_id_type=MESH).wait_recv()

    def own(u):
        chunk(u, me, xn, rn_sem).start()
        chunk(u, me, yn, rn_sem).start()
        chunk(u, me, sib, rs_sem).start()

    def forward(u):
        wait_chunks(u, 2, rn_sem)
        chunk(u, first, second, rd_sem).start()
        chunk(u, xn, sib, rs_sem).start()
        chunk(u, yn, sib, rs_sem).start()

    def diag(u):
        wait_chunks(u, 1, rd_sem)
        chunk(u, dg, sib, rs_sem).start()

    def arrived(u):
        wait_chunks(u, 4, rs_sem)

    f, d, o = forward, diag, own
    table = {
        "kv1": ([], [(o, 1)]),
        "q0": ([], [(f, 0), (o, 2)]),
        "q1": ([(o, 1)], []),
        "q2": ([], [(f, 1), (o, 3)]),
        "q3": ([(f, 0), (o, 2)], [(d, 0)]),
        "q4": ([(f, 1)], [(f, 2)]),
        "q5": ([(o, 3), (d, 0)], [(o, 4), (d, 1)]),
        "q6": ([(f, 2), (o, 4)], [(f, 3), (o, 5)]),
        "s0": ([(o, 5), (d, 1)], [(d, 2)]),
        "s1": ([(o, 6), (f, 3), (d, 2)], [(f, 4)]),
        "s2": ([(o, 7), (f, 4), (d, 3)], [(o, 6), (f, 5), (d, 3)]),
        "w0": ([(f, 5), (d, 4)], [(o, 7), (d, 4)]),
        "s3": ([], [(f, 6)]),
        "s4": ([(f, 6), (d, 5)], [(d, 5), (f, 7)]),
        "w1": ([(f, 7), (d, 6)], [(d, 6)]),
        "s6": ([(d, 7)], [(d, 7)]),
    }

    def slot(name):
        early, late = table.get(name, ([], []))
        def run(acts):
            with jax.named_scope(f"slot_{name}"):
                for act, u in acts:
                    act(u)

        if early == late:
            return run(early)
        for cond, acts in ((me < 2, early), (me >= 2, late)):
            if acts:
                pl.when(cond)(functools.partial(run, acts))

    def begin(us):
        with jax.named_scope("barrier"):
            pl.semaphore_wait(barrier, n - 1)
        seg_cp.wait()
        for k in range(1, n):
            seg_copy(k).start()
        for u in us:
            own(u)

    def keep_kv(i, r):
        for gg in range(2):
            for ab in range(2):
                piece = me if ab == 0 else 2 * n - 1 - me
                part = r[ab * HALF:(ab + 1) * HALF]
                kv_s[2 * i + gg, piece, 0] = part[:, gg * DH:(gg + 1) * DH].astype(BF16)
                kv_s[2 * i + gg, piece, 1] = jnp.transpose(part[:, (2 + gg) * DH:(3 + gg) * DH]).astype(BF16)

    with jax.named_scope("wait_x0"):
        x_copy(0).wait()
        wait(0)
        start(2)
    with jax.named_scope("kv0a"):
        y_s[0] = jnp.dot(x_s[:, :half_k], w_s[0, :half_k], preferred_element_type=F32)
    with jax.named_scope("wait_x1"):
        x_copy(1).wait()
        wait(1)
        start(3)
    with jax.named_scope("kv0b"):
        keep_kv(0, y_s[0] + jnp.dot(x_s[:, half_k:], w_s[0, half_k:], preferred_element_type=F32))
    pl.when(me >= 2)(functools.partial(begin, [0]))
    with jax.named_scope("wait_kv1"):
        wait(2)
        start(4)
        start(5)
    with jax.named_scope("kv1"):
        keep_kv(1, jnp.dot(x_s[...], w_s[1], preferred_element_type=F32))
    pl.when(me < 2)(functools.partial(begin, [0]))
    slot("kv1")

    n_l = n // 2
    n_h = n_l + 1
    n_a = me // 2 + 1

    def mixed(t):
        ab = jnp.where(t >= n_a, 1, 0)
        return ab, t + ab * (n_l - n_a)

    def mask_step(t):
        ab, kb = mixed(t - n_l)
        ab = jnp.where(t < n_l, 1, ab)
        kb = jnp.where(t < n_l, t, kb)
        qp = jnp.where(ab == 1, 2 * n - 1 - me, me)
        sq = seg_s[me, pl.ds(ab, 1), :]
        pos_q = qp * HALF + lax.broadcasted_iota(jnp.int32, (HALF, HALF), 1)
        for h in range(2):
            p = kb * 2 + h
            hi = jnp.where(p >= n, 1, 0)
            d = jnp.where(p >= n, 2 * n - 1 - p, p)
            sk = jnp.transpose(jnp.broadcast_to(seg_s[d, pl.ds(hi, 1), :], (HALF, HALF)))
            pos_k = p * HALF + lax.broadcasted_iota(jnp.int32, (HALF, HALF), 0)
            ok = (sk == sq) & (pos_k <= pos_q)
            b_s[t, h * HALF:(h + 1) * HALF, :] = jnp.where(ok, 0.0, -jnp.inf)

    def q_chunk(j):
        r = jnp.dot(x_s[...], w_s[2 + j], preferred_element_type=F32).astype(BF16)
        for hh in range(NC // DH):
            for ab in range(2):
                q_s[ab, j * (NC // DH) + hh] = r[ab * HALF:(ab + 1) * HALF, hh * DH:(hh + 1) * DH]

    nexts = [[6 + j] for j in range(n_q - 2)] + [[4 + n_q, 5 + n_q], [6 + n_q, 7 + n_q]]
    for j in range(n_q):
        with jax.named_scope(f"wait_q#j={j}"):
            wait(3 + j)
            for i in nexts[j]:
                start(i)
            if j == n_q - 2:
                seg_all().wait_recv()
        with jax.named_scope(f"q#j={j}"):
            if j >= n_q - 2:
                for t in range(n_l + n_h):
                    if (t < n_l) == (j == n_q - 2):
                        mask_step(t)
            q_chunk(j)
        slot(f"q{j}")
    for i in range(8 + n_q, 3 + 2 * n_q):
        start(i)

    o_s = x_s
    rows_g = g_sz * HALF
    scale = LOG2E * DH ** -0.5
    neg = -jnp.inf

    def fold(op, a):
        return op(a.reshape(a.shape[0] // 8, 8, HALF), axis=0)

    def across(op, a):
        return jnp.broadcast_to(op(a, axis=0, keepdims=True), a.shape)

    def heads(s, j):
        return s[:, j * HALF:(j + 1) * HALF]

    def probs(s, m):
        return jnp.exp2((s.reshape(s.shape[0] // 8, 8, HALF) - m[None]) * scale).reshape(s.shape)

    tiles = [range(lo, min(lo + 2, g_sz)) for lo in range(0, g_sz, 2)]

    def span(js):
        return slice(js[0] * HALF, (js[-1] + 1) * HALF)

    def q_of(ab, g, js):
        return q_s[ab, g * g_sz + js[0]:g * g_sz + js[-1] + 1].reshape(len(js) * HALF, DH)

    def scores_low(i, g, js):
        k = kv_s[g, 0:n, 0].reshape(n_l * KB, DH)
        s = lax.dot_general(k, q_of(1, g, js), (((1,), (1,)), ((), ())), preferred_element_type=F32)
        for jj, j in enumerate(js):
            mx = None
            for t in range(n_l):
                sj = heads(s[t * KB:(t + 1) * KB], jj) + b_s[t]
                s_s[i % 2, t, j] = sj
                f = fold(jnp.max, sj)
                mx = f if mx is None else jnp.maximum(mx, f)
            ml_s[g, j] = across(jnp.max, mx)

    def values_low(i, g, js):
        v = jnp.concatenate([kv_s[g, p, 1] for p in range(n)], axis=1)
        ps = []
        for j in js:
            m = ml_s[g, j]
            m = jnp.where(m == neg, 0.0, m)
            cols, tot = [], None
            for t in range(n_l):
                p = probs(s_s[i % 2, t, j], m)
                f = fold(jnp.sum, p)
                tot = f if tot is None else tot + f
                cols.append(p.astype(BF16))
            ll_s[g, j] = tot
            ps.append(jnp.concatenate(cols, axis=0))
        al_s[g, :, span(js)] = jnp.dot(v, jnp.concatenate(ps, axis=1), preferred_element_type=F32)

    order = [0, n_h - 1] + list(range(1, n_h - 1))
    every = range(g_sz)

    def scores_rest(i, g, t):
        ab, kb = (0, 0) if t == 0 else (1, n - 1 - me // 2) if t == n_h - 1 else mixed(t)
        k = kv_s[g, pl.ds(kb * 2, 2), 0].reshape(KB, DH)
        s = lax.dot_general(k, q_of(ab, g, every), (((1,), (1,)), ((), ())), preferred_element_type=F32)
        for j in every:
            sj = heads(s, j) + b_s[n_l + t]
            s_s[i % 2, t, j] = sj
            mx = fold(jnp.max, sj)
            if t == n_h - 1:
                mx = jnp.maximum(mx, ml_s[g, j])
            elif t > 0:
                mx = jnp.maximum(mx, m_s[g % 2, ab, j])
            m_s[g % 2, ab, j] = mx

    def scores_end(i, g):
        for ab in range(2):
            for j in every:
                m_s[g % 2, ab, j] = across(jnp.max, m_s[g % 2, ab, j])

    def values_rest(i, g, t):
        ab, kb = (0, 0) if t == 0 else (1, n - 1 - me // 2) if t == n_h - 1 else mixed(t)
        v = jnp.concatenate([kv_s[g, kb * 2, 1], kv_s[g, kb * 2 + 1, 1]], axis=1)
        ps, corrs = [], []
        for j in every:
            p = probs(s_s[i % 2, t, j], m_s[g % 2, ab, j])
            l = fold(jnp.sum, p)
            if t == n_h - 1:
                corrs.append(jnp.exp2((ml_s[g, j] - m_s[g % 2, 1, j]) * scale))
                l += ll_s[g, j] * corrs[-1]
            elif t > 0:
                l += l_s[ab, j]
            l_s[ab, j] = l
            ps.append(p.astype(BF16))
        a = jnp.dot(v, jnp.concatenate(ps, axis=1), preferred_element_type=F32)
        if t == n_h - 1:
            old = [(al_s[g, :, span([j])].reshape(DH // 8, 8, HALF) * corrs[j][None]).reshape(DH, HALF) for j in every]
            a += jnp.concatenate(old, axis=1)
        elif t > 0:
            a += a_s[ab]
        a_s[ab] = a

    def values_end(i, g):
        for ab in range(2):
            for j in every:
                r = 1.0 / jnp.sum(l_s[ab, j], axis=0, keepdims=True)
                o = jnp.transpose(a_s[ab, :, span([j])] * r).astype(BF16)
                o_s[ab * HALF:(ab + 1) * HALF, (g * g_sz + j) * DH:(g * g_sz + j + 1) * DH] = o

    def parts(i, low, rest, end):
        if i is None:
            return []
        ab, g = units[i]
        if ab == 0:
            return [functools.partial(low, i, g, js) for js in tiles]
        done = [functools.partial(end, i, g)]
        return [functools.partial(rest, i, g, t) for t in order] + done

    def block(i, j):
        if i is not None:
            with jax.named_scope(f"arrived#i={i}"):
                arrived(i)
        with jax.named_scope(f"block#s={i}#v={j}"):
            a = parts(i, scores_low, scores_rest, scores_end)
            b = parts(j, values_low, values_rest, values_end)
            for k in range(max(len(a), len(b))):
                for lst in (a, b):
                    if k < len(lst):
                        lst[k]()

    cuts = [min(g * g_sz * DH // KB * KB, d_model) for g in range(n_kv)] + [d_model]

    def project(g):
        if g == 0:
            with jax.named_scope("wait_wo"):
                for j in range(n_q):
                    wait(3 + n_q + j)
        rows = slice(cuts[g], cuts[g + 1])
        with jax.named_scope(f"wo#g={g}"):
            for j in range(n_q):
                y = jnp.dot(o_s[:, rows], w_s[j, rows, :], preferred_element_type=F32)
                if g > 0:
                    y += y_s[j]
                if g < n_kv - 1:
                    y_s[j] = y
                else:
                    y_ref[:, j * NC:(j + 1) * NC] = y.astype(BF16)

    block(0, None)
    slot("s0")
    for i in range(1, len(units)):
        block(i, i - 1)
        slot(f"s{i}")
        if i % 2 == 0:
            project(i // 2 - 1)
            slot(f"w{i // 2 - 1}")
    block(None, len(units) - 1)
    project(n_kv - 1)

    with jax.named_scope("tail"):
        seg_all().wait_send()
        ref = kv_s.at[:, pl.ds(0, 2 * (n - 1))]
        pltpu.make_async_remote_copy(
            src_ref=ref, dst_ref=ref, send_sem=send_sem, recv_sem=rs_sem.at[0],
            device_id={"cp": sib}, device_id_type=MESH).wait_send()


def solution(mesh):
    n = mesh.shape["cp"]

    def local(x, seg, wq, wk, wv, wo):
        lq, d = x.shape
        hq = wq.shape[1] // DH
        hkv = wk.shape[1] // DH
        g_sz = hq // hkv
        n_q = wq.shape[1] // NC
        dma = pltpu.SemaphoreType.DMA
        anyspec = pl.BlockSpec(memory_space=pl.ANY)
        return pl.pallas_call(
            functools.partial(_kernel, n, g_sz),
            out_shape=pltpu.VMEM((lq, wo.shape[1]), BF16),
            in_specs=[anyspec] * 6,
            out_specs=pl.BlockSpec(memory_space=pltpu.VMEM),
            scratch_shapes=[
                pltpu.VMEM((lq, d), BF16),
                pltpu.VMEM((n_q + 2, d, NC), BF16),
                pltpu.VMEM((hkv, 2 * n, 2, HALF, DH), BF16),
                pltpu.VMEM((2, hq, HALF, DH), BF16),
                pltpu.VMEM((2, n // 2 + 1, g_sz, KB, HALF), F32),
                pltpu.VMEM((n + 1, KB, HALF), F32),
                pltpu.VMEM((2, 2, g_sz, 8, HALF), F32),
                pltpu.VMEM((2, g_sz, 8, HALF), F32),
                pltpu.VMEM((2, DH, g_sz * HALF), F32),
                pltpu.VMEM((hkv, g_sz, 8, HALF), F32),
                pltpu.VMEM((hkv, g_sz, 8, HALF), F32),
                pltpu.VMEM((hkv, DH, g_sz * HALF), F32),
                pltpu.VMEM((n_q, lq, NC), F32),
                pltpu.VMEM((n, 2, HALF), jnp.int32),
                dma((2,)), dma((2 * n_q + 6,)), dma, dma,
                dma, dma((2 * hkv,)), dma((2 * hkv,)), dma((2 * hkv,)), dma,
            ],
            compiler_params=pltpu.CompilerParams(
                collective_id=0, has_side_effects=True, vmem_limit_bytes=60 * 2 ** 20),
            name="layer",
        )(x, seg.reshape(2, HALF), wq, wk, wv, wo)

    rows = P(("dp", "cp"), None)
    return jax.shard_map(local, mesh=mesh, in_specs=(rows, P(("dp", "cp")), P(), P(), P(), P()), out_specs=rows, check_vma=False)
```
